32 devices in a mesh: dp: 4 (over x, core), tensor: 8 (over z, y).
Axes of the slice: x: 2, y: 2, z: 4, core: 2. Of those that a mesh axis runs over, the one named last changes fastest.
Arguments:
- tokens: bfloat16 [96, 8, 4096], P('dp'), may hold values from -6 to 6
- norm_gain: float32 [4096], replicated, may hold values from 0.1 to 1.9
- in_weight: bfloat16 [4096, 2, 4096], P(None, None, 'tensor'), may hold values from -0.09375 to 0.09375
- group_weight: bfloat16 [4096, 1024], P(None, 'tensor'), may hold values from -0.09375 to 0.09375
- step_weight: bfloat16 [4096, 64], P(None, 'tensor'), may hold values from -0.09375 to 0.09375
- value_kernel: bfloat16 [4, 4096], P(None, 'tensor'), may hold values from -3 to 3
- value_offset: bfloat16 [4096], P('tensor'), may hold values from -3 to 3
- group_kernel: bfloat16 [4, 1024], P(None, 'tensor'), may hold values from -3 to 3
- group_offset: bfloat16 [1024], P('tensor'), may hold values from -3 to 3
- step_bias: float32 [64], P('tensor'), may hold values from -4 to 1
- decay_rate: float32 [64], P('tensor'), may hold values from 0.05 to 2
- skip_gain: float32 [64], P('tensor'), may hold values from 0.5 to 2
- out_gain: float32 [4096], P('tensor'), may hold values from 0.1 to 1.9
- out_weight: bfloat16 [4096, 4096], P('tensor'), may hold values from -0.09375 to 0.09375
- scan_state: bfloat16 [96, 64, 64, 128], P('dp', 'tensor'), may hold values from -6 to 6
- value_cache: bfloat16 [96, 3, 4096], P('dp', None, 'tensor'), may hold values from -6 to 6
- group_cache: bfloat16 [96, 3, 1024], P('dp', None, 'tensor'), may hold values from -6 to 6
- accepted: int32 [96], P('dp'), may hold values from 0 to 8, as said below
- draft_lengths: int32 [96], P('dp'), may hold values from 1 to 8, as said below
- live_flags: int32 [96], P('dp'), may hold values 0 or 1
Outputs:
- layer_out: bfloat16 [96, 8, 4096], P('dp')
- kept_state: bfloat16 [96, 64, 64, 128], P('dp', 'tensor')
- value_kept: bfloat16 [96, 3, 4096], P('dp', None, 'tensor')
- group_kept: bfloat16 [96, 3, 1024], P('dp', None, 'tensor')
- accepted_total: int32 [1], replicated
The draws below stay inside these ranges and needn't reach their ends.
Inputs may be any that keep to these rules, and one draw needn't show every extreme that they name: `draft_lengths`: positions at or after a request's draft length are padding. `accepted`: never more than the same request's draft length.
All inputs are finite; a program needn't handle non-finite values.
Results may differ from the reference program's by a relative error of at most 0.012.
Values may be sent and summed in bfloat16 or wider, within the bound.
A program may use at most 128 MiB of HBM per device.

```python
import math
import jax
import jax.numpy as jnp
from jax import lax

D = 4096
STATE = 128
HEADDIM = 64
CONV = 4
DRAFT = 8
REQ_DEV = 24
HEADS = 64
NGROUPS = 4
INNER = 4096
GCOLS = 1024
REQUESTS = 96


def draft_pair(key):
    block_count = REQUESTS // REQ_DEV
    full_row = jax.random.randint(jax.random.fold_in(key, 10), (), 0, REQUESTS)
    short_row = (full_row + 1) % REQUESTS
    block_caps = jax.random.randint(jax.random.fold_in(key, 11), (block_count,), 1, DRAFT + 1)
    block_caps = jnp.where(jnp.arange(block_count) == full_row // REQ_DEV, DRAFT, block_caps)
    per_request = jnp.repeat(block_caps, REQ_DEV, total_repeat_length=REQUESTS)
    lengths = jax.random.randint(jax.random.fold_in(key, 12), (REQUESTS,), 1, per_request + 1)
    row_ids = jnp.arange(REQUESTS)
    lengths = jnp.where(row_ids == full_row, DRAFT, lengths)
    lengths = jnp.where(row_ids == short_row, 1, lengths)
    accepted_counts = jax.random.randint(jax.random.fold_in(key, 13), (REQUESTS,), 0, lengths + 1)
    accepted_counts = jnp.where(row_ids == full_row, DRAFT, accepted_counts)
    accepted_counts = jnp.where(row_ids == short_row, 0, accepted_counts)
    return (lengths.astype(jnp.int32), accepted_counts.astype(jnp.int32))


def draw_draft_lengths(key, part):
    return draft_pair(key)[0]


def draw_accepted(key, part):
    return draft_pair(key)[1]


def plant(array, own_key, smallest, largest):
    extent = array.shape
    index_at = [jax.random.randint(jax.random.fold_in(own_key, axis), (), 0, extent[axis]) for axis in range(len(extent))]
    array = array.at[tuple(index_at)].set(smallest)
    longest = extent.index(max(extent))
    index_at[longest] = (index_at[longest] + 1) % extent[longest]
    return array.at[tuple(index_at)].set(largest)


def block_levels(own_key, dims, cuts, smallest, top_value):
    factor_of, own = 1.0, jax.random.fold_in(own_key, 6)
    for dim, blocks in cuts:
        draws = jnp.exp(jax.random.uniform(jax.random.fold_in(own, dim), (blocks,), jnp.float32, smallest / len(cuts), top_value / len(cuts)))
        factor_of = factor_of * jnp.repeat(draws, dims[dim] // blocks).reshape([-1 if axis == dim else 1 for axis in range(len(dims))])
    return factor_of


def noise(own_key, dims, deviation, most, cuts=(), kind=jnp.bfloat16):
    factor_of = block_levels(own_key, dims, cuts, -0.22, 0.18) if cuts else 1.0
    result = jax.random.normal(own_key, dims, jnp.float32) * deviation * factor_of
    return jnp.minimum(jnp.maximum(result, -most), most).astype(kind)


def setup_inputs(seed: int = 0) -> dict:
    arg_keys = jax.random.split(jax.random.key(seed), 21)
    tokens = noise(arg_keys[0], (REQUESTS, DRAFT, D), 1.0, 6.0, ((0, 4),))
    norm_gain = jnp.clip(1.0 + 0.18 * jax.random.normal(arg_keys[1], (D,), jnp.float32), 0.1, 1.9)
    in_weight = noise(arg_keys[2], (D, 2, INNER), D ** -0.5, 0.09375, ((2, 8),))
    group_weight = noise(arg_keys[3], (D, GCOLS), D ** -0.5, 0.09375, ((1, 8),))
    step_weight = noise(arg_keys[4], (D, HEADS), D ** -0.5, 0.09375, ((1, 8),))
    value_kernel = noise(arg_keys[5], (CONV, INNER), CONV ** -0.5, 3.0, ((1, 8),))
    value_offset = noise(arg_keys[6], (INNER,), 0.5, 3.0, ((0, 8),))
    group_kernel = noise(arg_keys[7], (CONV, GCOLS), CONV ** -0.5, 3.0, ((1, 8),))
    group_offset = noise(arg_keys[8], (GCOLS,), 0.5, 3.0, ((0, 8),))
    step_bias = jnp.clip(-4.0 + 5.0 * jax.random.uniform(arg_keys[9], (HEADS,), jnp.float32) ** block_levels(arg_keys[9], (HEADS,), ((0, 8),), -0.2, 0.2), -4.0, 1.0)
    decay_rate = jnp.clip(jnp.exp(math.log(2.0) - 3.6888794 * jax.random.uniform(arg_keys[10], (HEADS,), jnp.float32) ** block_levels(arg_keys[10], (HEADS,), ((0, 8),), -0.2, 0.2)), 0.05, 2.0)
    skip_gain = jnp.clip(0.5 + 1.5 * jax.random.uniform(arg_keys[11], (HEADS,), jnp.float32) ** block_levels(arg_keys[11], (HEADS,), ((0, 8),), -0.2, 0.2), 0.5, 2.0)
    out_gain = jnp.clip(1.0 + 0.18 * jax.random.normal(arg_keys[12], (INNER,), jnp.float32), 0.1, 1.9)
    out_weight = noise(arg_keys[13], (INNER, D), INNER ** -0.5, 0.09375, ((0, 8),))
    scan_state = noise(arg_keys[14], (REQUESTS, HEADS, HEADDIM, STATE), 1.0, 6.0, ((0, 4), (1, 8)))
    value_cache = noise(arg_keys[15], (REQUESTS, CONV - 1, INNER), 1.0, 6.0, ((0, 4), (2, 8)))
    group_cache = noise(arg_keys[16], (REQUESTS, CONV - 1, GCOLS), 1.0, 6.0, ((0, 4), (2, 8)))
    accepted = draw_accepted(jax.random.fold_in(arg_keys[20], 71), 0)
    draft_lengths = draw_draft_lengths(jax.random.fold_in(arg_keys[20], 71), 0)
    live_flags = plant((jax.random.randint(arg_keys[19], (REQUESTS,), 0, 8) < 7).astype(jnp.int32), jax.random.fold_in(arg_keys[19], 1), 0, 1)
    return {"tokens": tokens, "norm_gain": norm_gain, "in_weight": in_weight, "group_weight": group_weight, "step_weight": step_weight, "value_kernel": value_kernel, "value_offset": value_offset, "group_kernel": group_kernel, "group_offset": group_offset, "step_bias": step_bias, "decay_rate": decay_rate, "skip_gain": skip_gain, "out_gain": out_gain, "out_weight": out_weight, "scan_state": scan_state, "value_cache": value_cache, "group_cache": group_cache, "accepted": accepted, "draft_lengths": draft_lengths, "live_flags": live_flags}


EPSILON = 1e-05

def convolve(window, fresh_rows, kernel, offset):
    sequence = jnp.concatenate([window, fresh_rows], axis=1)
    length = fresh_rows.shape[1]
    summed = jnp.zeros(fresh_rows.shape, jnp.float32) + offset.astype(jnp.float32)
    for tap_index in range(kernel.shape[0]):
        summed = summed + kernel[tap_index].astype(jnp.float32) * sequence[:, tap_index:tap_index + length].astype(jnp.float32)
    return (jax.nn.silu(summed), sequence)

def keep_window(sequence, kept_count, width_rows):
    return jax.vmap(lambda single, start_row: lax.dynamic_slice_in_dim(single, start_row, width_rows, 0))(sequence, kept_count)

def reference(tokens, norm_gain, in_weight, group_weight, step_weight, value_kernel, value_offset, group_kernel, group_offset, step_bias, decay_rate, skip_gain, out_gain, out_weight, scan_state, value_cache, group_cache, accepted, draft_lengths, live_flags):
    flat_rows = tokens.reshape(REQUESTS * DRAFT, D).astype(jnp.float32)
    normed = (flat_rows * lax.rsqrt(lax.optimization_barrier(jnp.mean(flat_rows * flat_rows, axis=1, keepdims=True)) + EPSILON) * norm_gain).astype(jnp.bfloat16)
    inner_proj = jnp.dot(normed, in_weight.reshape(D, 2 * INNER), preferred_element_type=jnp.float32).astype(jnp.bfloat16).reshape(REQUESTS, DRAFT, 2, INNER)
    gate_part = inner_proj[:, :, 0]
    value_part = inner_proj[:, :, 1]
    group_proj = jnp.dot(normed, group_weight, preferred_element_type=jnp.float32).astype(jnp.bfloat16).reshape(REQUESTS, DRAFT, GCOLS)
    step_raw = jnp.dot(normed, step_weight, preferred_element_type=jnp.float32).reshape(REQUESTS, DRAFT, HEADS)
    value_conv, value_seq = convolve(value_cache, value_part, value_kernel, value_offset)
    group_conv, group_seq = convolve(group_cache, group_proj, group_kernel, group_offset)
    group_maps = group_conv.reshape(REQUESTS, DRAFT, NGROUPS, 2, STATE)
    input_maps = group_maps[:, :, :, 0]
    output_maps = group_maps[:, :, :, 1]
    step_size = jax.nn.softplus(step_raw + step_bias)
    decay_step = jnp.exp(-step_size * decay_rate)
    kept_count = accepted * live_flags
    per_group = HEADS // NGROUPS

    def head_scan(head_index):
        values = lax.dynamic_slice_in_dim(value_conv, head_index * HEADDIM, HEADDIM, 2)
        group_index = head_index // per_group
        input_map = lax.dynamic_index_in_dim(input_maps, group_index, 2, keepdims=False)
        output_map = lax.dynamic_index_in_dim(output_maps, group_index, 2, keepdims=False)
        head_decay = lax.dynamic_index_in_dim(decay_step, head_index, 2, keepdims=False)
        head_step = lax.dynamic_index_in_dim(step_size, head_index, 2, keepdims=False)
        initial = lax.dynamic_index_in_dim(scan_state, head_index, 1, keepdims=False).astype(jnp.float32)
        head_skip = lax.dynamic_index_in_dim(skip_gain, head_index, 0, keepdims=False)

        def advance(carry_pair, position):
            current, kept_now = carry_pair
            scaled = (head_step[:, position][:, None] * values[:, position])[:, :, None]
            current = head_decay[:, position][:, None, None] * current + scaled * input_map[:, position][:, None, :]
            produced = lax.optimization_barrier(jnp.sum(current * output_map[:, position][:, None, :], axis=2)) + head_skip * values[:, position]
            kept_now = jnp.where((position < kept_count)[:, None, None], current, kept_now)
            return ((current, kept_now), produced)
        (final_state, kept_now), produced = lax.scan(advance, (initial, initial), jnp.arange(DRAFT, dtype=jnp.int32))
        return (produced, kept_now.astype(jnp.bfloat16))
    produced, kept_heads = lax.map(head_scan, jnp.arange(HEADS, dtype=jnp.int32))
    head_out = jnp.transpose(produced, (2, 1, 0, 3)).reshape(REQUESTS, DRAFT, INNER)
    kept_state = jnp.transpose(kept_heads, (1, 0, 2, 3))
    gated = head_out * jax.nn.silu(gate_part.astype(jnp.float32))
    grouped = gated.reshape(REQUESTS, DRAFT, NGROUPS, INNER // NGROUPS)
    scale_rows = lax.rsqrt(lax.optimization_barrier(jnp.mean(grouped * grouped, axis=3, keepdims=True)) + EPSILON)
    valid_rows = (jnp.arange(DRAFT)[None, :] < draft_lengths[:, None]) & (live_flags[:, None] == 1)
    normalized = jnp.where(valid_rows[:, :, None], (grouped * scale_rows).reshape(REQUESTS, DRAFT, INNER) * out_gain, 0.0).astype(jnp.bfloat16)
    layer_out = jnp.dot(normalized.reshape(REQUESTS * DRAFT, INNER), out_weight, preferred_element_type=jnp.float32).astype(jnp.bfloat16).reshape(REQUESTS, DRAFT, D)
    value_kept = keep_window(value_seq, kept_count, CONV - 1)
    group_kept = keep_window(group_seq, kept_count, CONV - 1)
    accepted_total = jnp.sum(kept_count).astype(jnp.int32).reshape(1)
    return (layer_out, kept_state, value_kept, group_kept, accepted_total)
```

```python
import jax
import jax.numpy as jnp
from jax import lax
from jax.experimental import pallas as pl
from jax.experimental.pallas import tpu as pltpu
from jax.sharding import PartitionSpec as P

EPSILON = 1e-05
MESH = pl.DeviceIdType.MESH
F32 = jnp.float32
BF16 = jnp.bfloat16


def iota(shape, axis):
    return lax.broadcasted_iota(jnp.int32, shape, axis)


def dot(a, b):
    return jnp.dot(a, b, preferred_element_type=F32)


def dot_nt(a, b):
    return lax.dot_general(a, b, (((1,), (1,)), ((), ())), preferred_element_type=F32)


def dot_tn(a, b):
    return lax.dot_general(a, b, (((0,), (0,)), ((), ())), preferred_element_type=F32)


def dot_split(a, b):
    high = a.astype(BF16)
    low = (a - high.astype(F32)).astype(BF16)
    return dot(high, b) + dot(low, b)


def silu(v):
    return v * (1.0 / (1.0 + jnp.exp(-v)))


def spread_cache(cache, rows, positions, first):
    depth, requests, width = cache.shape
    flat = cache.reshape(depth * requests, width)
    row = iota((rows, depth * requests), 0)
    col = iota((rows, depth * requests), 1)
    place = row % positions - (positions - depth)
    chosen = (col == place * requests + first + row // positions) & (place >= 0)
    return dot(chosen.astype(BF16), flat)


def convolve(fresh, cached, kernel, offset, positions):
    rows, width = fresh.shape
    taps = kernel.shape[0]
    fresh = fresh.reshape(rows // positions, positions, width)
    cached = cached.reshape(rows // positions, positions, width)
    place = iota(fresh.shape, 1)
    total = offset[None] + kernel[taps - 1 : taps][None] * fresh
    for shift in range(1, taps):
        merged = jnp.where(place < positions - shift, fresh, cached)
        moved = pltpu.roll(merged, shift, axis=1)
        total = total + kernel[taps - 1 - shift : taps - shift][None] * moved
    return silu(total).reshape(rows, width)


def prepare_kernel(
    accepted_hbm,
    draft_hbm,
    live_hbm,
    tokens_hbm,
    gain_hbm,
    weight_hbm,
    step_weight_hbm,
    cache_hbm,
    kernel_hbm,
    offset_hbm,
    bias_hbm,
    rate_hbm,
    normed_ref,
    conv_ref,
    mix_ref,
    keep_ref,
    after_ref,
    scale_ref,
    valid_ref,
    fresh_pick_ref,
    cache_pick_ref,
    group_kept_hbm,
    total_ref,
    accepted_ref,
    draft_ref,
    live_ref,
    tokens_ref,
    gain_ref,
    weight_ref,
    step_weight_ref,
    cache_ref,
    kernel_ref,
    offset_ref,
    bias_ref,
    rate_ref,
    group_kept_ref,
    load_sems,
    kept_sem,
):
    sources = (gain_hbm, tokens_hbm, weight_hbm, step_weight_hbm, cache_hbm)
    sources += (kernel_hbm, offset_hbm, bias_hbm, rate_hbm, accepted_hbm, draft_hbm, live_hbm)
    targets = (gain_ref, tokens_ref, weight_ref, step_weight_ref, cache_ref)
    targets += (kernel_ref, offset_ref, bias_ref, rate_ref, accepted_ref, draft_ref, live_ref)
    loads = [
        pltpu.make_async_copy(source, target, load_sems.at[index])
        for index, (source, target) in enumerate(zip(sources, targets))
    ]
    for load in loads:
        load.start()
    rows, model_width = tokens_ref.shape
    requests = accepted_ref.shape[0]
    positions = rows // requests
    heads = bias_ref.shape[1]
    depth = cache_ref.shape[0]
    lanes = positions * heads
    step = 16 if rows % 16 == 0 else 8
    loads[0].wait()
    loads[1].wait()
    for start in range(0, rows, step):
        wide = tokens_ref[start : start + step].astype(F32)
        mean = jnp.sum(wide * wide, axis=1, keepdims=True) / model_width
        normed_ref[start : start + step] = (
            wide * lax.rsqrt(mean + EPSILON) * gain_ref[...]
        ).astype(BF16)
    for load in loads[2:]:
        load.wait()
    normed = normed_ref[...]
    group_proj = dot(normed, weight_ref[...]).astype(BF16)
    step_raw = dot_nt(normed, step_weight_ref[...])

    cache = cache_ref[...]
    cached = spread_cache(cache, rows, positions, 0)
    conv = convolve(
        group_proj.astype(F32),
        cached,
        kernel_ref[...].astype(F32),
        offset_ref[...].astype(F32),
        positions,
    )
    conv_ref[...] = conv.astype(BF16)

    counts = [accepted_ref[r] * live_ref[r] for r in range(requests)]
    total = counts[0]
    for count in counts[1:]:
        total = total + count
    total_ref[...] = jnp.full(total_ref.shape, total, jnp.int32)

    bias = jnp.concatenate([bias_ref[...]] * positions, axis=1)[None]
    rate = jnp.concatenate([rate_ref[...]] * positions, axis=1)[None]
    raw = jnp.concatenate([step_raw] * positions, axis=1).reshape(requests, positions, lanes)
    raw = raw + bias
    size = jnp.maximum(raw, 0.0) + jnp.log1p(jnp.exp(-jnp.abs(raw)))
    log_decay = -size * rate
    place = iota((requests, positions, lanes), 1)
    source = iota((requests, positions, lanes), 2) // heads
    after = log_decay
    shift = 1
    while shift < positions:
        after = after + jnp.where(place >= shift, pltpu.roll(after, shift, axis=1), 0.0)
        shift *= 2
    kept = jnp.stack([jnp.full((positions, lanes), count, jnp.int32) for count in counts])
    own = place == source
    after_source = jnp.sum(jnp.where(own, after, 0.0), axis=1, keepdims=True)
    size_source = jnp.sum(jnp.where(own, size, 0.0), axis=1, keepdims=True)
    causal = place >= source
    mix = jnp.where(causal, jnp.exp(jnp.where(causal, after - after_source, 0.0)), 0.0) * size_source
    kept_after = jnp.sum(jnp.where(place == kept - 1, after, 0.0), axis=1, keepdims=True)
    before = place < kept
    keep = jnp.where(before, jnp.exp(jnp.where(before, kept_after - after, 0.0)), 0.0) * size
    mix_ref[...] = mix.reshape(rows, lanes)
    keep_ref[...] = keep.reshape(rows, lanes)
    after_ref[...] = jnp.exp(after).reshape(rows, lanes)
    scale_ref[...] = jnp.exp(kept_after[:, 0, :heads])

    wide_lanes = valid_ref.shape[1]
    drafted = jnp.stack(
        [
            jnp.full((positions, wide_lanes), draft_ref[r] * (live_ref[r] == 1).astype(jnp.int32), jnp.int32)
            for r in range(requests)
        ]
    )
    valid = iota(drafted.shape, 1) < drafted
    valid_ref[...] = valid.astype(F32).reshape(rows, wide_lanes)

    def picks(width, position_of, request_of):
        shape = (requests, width)
        row = iota(shape, 0)
        count = jnp.zeros(shape, jnp.int32)
        for r in range(requests):
            count = jnp.where(row == r, counts[r], count)
        col = iota(shape, 1)
        return jnp.concatenate(
            [
                ((position_of(col) == count + t) & (request_of(col) == row)).astype(F32)
                for t in range(depth)
            ],
            axis=0,
        ).astype(BF16)

    fresh_pick = picks(rows, lambda col: col % positions + depth, lambda col: col // positions)
    cache_pick = picks(depth * requests, lambda col: col // requests, lambda col: col % requests)
    fresh_pick_ref[...] = fresh_pick
    cache_pick_ref[...] = cache_pick
    kept_rows = dot(fresh_pick, group_proj) + dot(cache_pick, cache.reshape(depth * requests, -1))
    group_kept_ref[...] = kept_rows.reshape(group_kept_ref.shape).astype(BF16)
    kept_copy = pltpu.make_async_copy(group_kept_ref, group_kept_hbm, kept_sem)
    kept_copy.start()
    kept_copy.wait()


def layer_kernel(
    scale_ref,
    skip_ref,
    inner_ref,
    conv_ref,
    mix_ref,
    keep_ref,
    after_ref,
    valid_ref,
    cache_ref,
    kernel_ref,
    offset_ref,
    gain_ref,
    count_ref,
    weight_hbm,
    state_hbm,
    out_buf,
    kept_buf,
    total_ref,
    weight_buf,
    state_buf,
    y_send,
    y_recv,
    z_send,
    z_recv,
    acc_buf,
    place_buf,
    map_recv,
    input_map,
    output_map,
    weighted_buf,
    sq_send,
    sq_recv,
    count_recv,
    weight_sem,
    state_sem,
    map_sems,
    sq_sems,
    y_sems,
    z_sems,
    o_sems,
    p_sems,
    count_sems,
):
    chunks, height, half = y_send.shape
    rows, inner = inner_ref.shape[1:]
    requests = state_buf.shape[0]
    positions = rows // requests
    lanes = mix_ref.shape[1]
    heads = lanes // positions
    head_dim = inner // heads
    per_chunk = requests // chunks
    depth = cache_ref.shape[0]

    members = lax.axis_size("tensor")
    fars = members // 2
    width = half // fars
    me = lax.axis_index("tensor")
    far, near = me // 2, me % 2
    partner = far * 2 + (1 - near)

    def far_at(step):
        return lax.rem(far + 1 + step, fars)

    def far_of(step):
        return lax.rem(far - 1 - step + 2 * fars, fars)

    groups = lax.axis_size("dp")
    group = lax.axis_index("dp")

    def cols(start, width):
        return pl.ds(pl.multiple_of(start, width), width)

    weight_loads = [
        pltpu.make_async_copy(
            weight_hbm.at[:, cols(block * half, half)],
            weight_buf.at[slot],
            weight_sem.at[slot],
        )
        for slot, block in enumerate((1 - near, near))
    ]
    state_loads = [
        pltpu.make_async_copy(
            state_hbm.at[pl.ds(c * per_chunk, per_chunk)],
            state_buf.at[pl.ds(c * per_chunk, per_chunk)],
            state_sem.at[c],
        )
        for c in range(chunks)
    ]
    state_loads[0].start()
    weight_loads[0].start()
    weight_loads[1].start()
    for load in state_loads[1:]:
        load.start()

    barrier = pltpu.get_barrier_semaphore()
    pl.semaphore_signal(barrier, inc=1, device_id={"tensor": partner}, device_id_type=MESH)

    for step in range(fars - 1):
        pl.semaphore_signal(
            barrier, inc=1, device_id={"tensor": far_at(step) * 2 + near}, device_id_type=MESH
        )
    for hop in range(groups - 1):
        pl.semaphore_signal(
            barrier,
            inc=1,
            device_id={"dp": lax.rem(group + 1 + hop, groups)},
            device_id_type=MESH,
        )
    pl.semaphore_wait(barrier, fars + groups - 1)

    def remote(source, target, sems, index, device):
        return pltpu.make_async_remote_copy(
            src_ref=source,
            dst_ref=target,
            send_sem=sems.at[0, index],
            recv_sem=sems.at[1, index],
            device_id={"tensor": device},
            device_id_type=MESH,
        )

    map_copy = remote(conv_ref, map_recv, map_sems, 0, partner)
    map_copy.start()
    count_copies = []
    for hop in range(groups - 1):
        copy = pltpu.make_async_remote_copy(
            src_ref=count_ref,
            dst_ref=count_recv.at[hop],
            send_sem=count_sems.at[0, hop],
            recv_sem=count_sems.at[1, hop],
            device_id={"dp": lax.rem(group + 1 + hop, groups)},
            device_id_type=MESH,
        )
        copy.start()
        count_copies.append(copy)

    shape = (lanes, inner)
    target_head = iota(shape, 1) // head_dim
    lane_row = iota(shape, 0)
    for j in range(positions):
        place_buf[j] = (lane_row == target_head + j * heads).astype(F32).astype(BF16)
    to_heads = place_buf[0]

    lane_head = iota((1, inner), 1) // head_dim
    skip = jnp.zeros((1, inner), F32)
    for h in range(heads):
        skip = jnp.where(lane_head == h, skip_ref[h], skip)

    cache = cache_ref[...]
    kernel = kernel_ref[...].astype(F32)
    offset = offset_ref[...].astype(F32)

    def values_of(c):
        span = slice(c * height, (c + 1) * height)
        cached = spread_cache(cache, height, positions, c * per_chunk)
        return convolve(inner_ref[1, span].astype(F32), cached, kernel, offset, positions)

    def wait_maps():
        map_copy.wait_recv()
        mine = conv_ref[...].astype(F32)
        other = map_recv[...].astype(F32)
        even = near == 0
        input_map[...] = jnp.where(even, mine, other)
        output_map[...] = jnp.where(even, other, mine)

    def front(c):
        span = slice(c * height, (c + 1) * height)
        values = values_of(c)
        gate = silu(inner_ref[0, span].astype(F32))
        if c == 0:
            wait_maps()
        outputs = output_map[span].astype(BF16)
        inputs = input_map[span].astype(BF16)
        align = dot_nt(outputs, inputs)
        square = (height, height)
        same = iota(square, 0) // positions == iota(square, 1) // positions
        fold = (height, lanes)
        folded = (iota(fold, 0) % positions == iota(fold, 1) // heads).astype(F32).astype(BF16)
        mix = (mix_ref[span] * dot_split(jnp.where(same, align, 0.0), folded)).astype(BF16)
        values3 = values.reshape(per_chunk, positions, inner)
        head = skip * values
        for j in range(positions):
            spread = jnp.broadcast_to(values3[:, j : j + 1], values3.shape).reshape(height, inner)
            head = head + dot(mix, place_buf[j]) * spread
        state_loads[c].wait()
        carried = jnp.concatenate(
            [
                dot_nt(
                    output_map[r * positions : (r + 1) * positions].astype(BF16), state_buf[r]
                )
                for r in range(c * per_chunk, (c + 1) * per_chunk)
            ],
            axis=0,
        )
        head = head + carried * dot_split(after_ref[span], to_heads)
        gated = head * gate
        squares = jnp.sum(gated * gated, axis=1, keepdims=True)
        sq_send[c] = jnp.broadcast_to(squares, sq_send.shape[1:])
        sq_copies[c].start()
        weighted_buf[span] = values * dot_split(keep_ref[span], to_heads)
        return (gated * gain_ref[...]).astype(BF16)

    sq_copies = [
        remote(sq_send.at[c], sq_recv.at[c], sq_sems, c, partner) for c in range(chunks)
    ]
    y_copies = [remote(y_send.at[c], y_recv.at[c], y_sems, c, partner) for c in range(chunks)]
    z_copies = [
        [
            remote(
                z_send.at[c, step],
                z_recv.at[c, step],
                z_sems,
                c * (fars - 1) + step,
                far_at(step) * 2 + near,
            )
            for step in range(fars - 1)
        ]
        for c in range(chunks)
    ]

    def region(c, plane, owner):
        return out_buf.at[pl.ds(c * height, height), cols(plane * half + owner * width, width)]

    def owned(c, owner, sems, index, device, plane=near):
        return remote(region(c, plane, owner), region(c, plane, owner), sems, index, device)

    def send_partial(c):
        rows_in = front(c)
        if c == 0:
            weight_loads[0].wait()
        y_send[c] = dot(rows_in, weight_buf[0]).astype(BF16)
        y_copies[c].start()
        if c == 0:
            weight_loads[1].wait()
        acc_buf[c] = dot(rows_in, weight_buf[1])

    def pair_sum(c):
        span = slice(c * height, (c + 1) * height)
        sq_copies[c].wait_recv()
        total = (sq_send[c] + sq_recv[c])[:, :1] / (2 * inner)
        scale = lax.rsqrt(total + EPSILON) * valid_ref[span, :1]
        y_copies[c].wait_recv()
        acc_buf[c] = (acc_buf[c] + y_recv[c].astype(F32)) * scale

        for step in range(fars - 1):
            z_send[c, step] = acc_buf[c, :, cols(far_at(step) * width, width)].astype(BF16)
            z_copies[c][step].start()

    sent = []

    def send_final(c):
        total = acc_buf[c, :, cols(far * width, width)]
        for step in range(fars - 1):
            z_copies[c][step].wait_recv()
            total = total + z_recv[c, step].astype(F32)
        span = pl.ds(c * height, height)
        out_buf[span, cols(near * half + far * width, width)] = total.astype(BF16)
        copies = [owned(c, far, p_sems, c * fars, partner)]
        for step in range(fars - 1):
            index = c * (fars - 1) + step
            copies.append(owned(c, far, o_sems, index, far_at(step) * 2 + near))
        for copy in copies:
            copy.start()
            sent.append(copy)

    def forward(c):
        for step in range(fars - 1):
            index = c * (fars - 1) + step
            owned(c, far_of(step), o_sems, index, partner).wait_recv()
            copy = owned(c, far_of(step), p_sems, c * fars + 1 + step, partner)
            copy.start()
            sent.append(copy)

    def complete(c):
        owned(c, far, p_sems, c * fars, partner, 1 - near).wait_recv()
        for step in range(fars - 1):
            index = c * fars + 1 + step
            owned(c, far_of(step), p_sems, index, partner, 1 - near).wait_recv()

    def keep_state(c):
        for r in range(c * per_chunk, (c + 1) * per_chunk):
            span = slice(r * positions, (r + 1) * positions)
            added = dot_tn(weighted_buf[span].astype(BF16), input_map[span].astype(BF16))
            for h in range(heads):
                block = slice(h * head_dim, (h + 1) * head_dim)
                kept_buf[r, block] = (
                    scale_ref[r, h] * state_buf[r, block].astype(F32) + added[block]
                ).astype(BF16)

    stages = (
        (send_partial, 0),
        (pair_sum, 2),
        (send_final, 4),
        (forward, 6),
        (keep_state, 4),
        (complete, 9),
    )
    for slot in range(chunks + max(lag for _, lag in stages)):
        for stage, lag in stages:
            if 0 <= slot - lag < chunks:
                stage(slot - lag)

    count = count_ref[...]
    for hop in range(groups - 1):
        count_copies[hop].wait_recv()
        count = count + count_recv[hop]
    total_ref[0] = count[0, 0]

    for copy in [map_copy] + sq_copies + y_copies + sum(z_copies, []) + sent + count_copies:
        copy.wait_send()


def finish_kernel(
    rows_ref,
    kept_ref,
    inner_ref,
    cache_ref,
    fresh_pick_ref,
    cache_pick_ref,
    rows_hbm,
    kept_hbm,
    value_kept_hbm,
    value_kept_ref,
    sems,
):
    copies = [
        pltpu.make_async_copy(rows_ref, rows_hbm, sems.at[0]),
        pltpu.make_async_copy(kept_ref, kept_hbm, sems.at[1]),
        pltpu.make_async_copy(value_kept_ref, value_kept_hbm, sems.at[2]),
    ]
    copies[0].start()
    copies[1].start()
    depth, requests, inner = cache_ref.shape
    cache_rows = cache_ref[...].reshape(depth * requests, inner)
    value_kept = dot(fresh_pick_ref[...], inner_ref[1]) + dot(cache_pick_ref[...], cache_rows)
    value_kept_ref[...] = value_kept.reshape(value_kept_ref.shape).astype(BF16)
    copies[2].start()
    for copy in copies:
        copy.wait()


def local(
    tokens,
    norm_gain,
    in_weight,
    group_weight,
    step_weight,
    value_kernel,
    value_offset,
    group_kernel,
    group_offset,
    step_bias,
    decay_rate,
    skip_gain,
    out_gain,
    out_weight,
    scan_state,
    value_cache,
    group_cache,
    accepted,
    draft_lengths,
    live_flags,
):
    requests, positions, model_width = tokens.shape
    rows = requests * positions
    heads, head_dim, state_size = scan_state.shape[1:]
    inner = heads * head_dim
    map_width = group_weight.shape[1]
    depth = value_cache.shape[1]
    lanes = positions * heads
    groups = lax.axis_size("dp")
    chunks = next(c for c in (6, 4, 3, 2, 1) if requests % c == 0 and (rows // c) % 16 == 0)
    height = rows // chunks
    half = model_width // 2
    vmem = pl.BlockSpec(memory_space=pltpu.VMEM)
    smem = pl.BlockSpec(memory_space=pltpu.SMEM)
    hbm = pl.BlockSpec(memory_space=pltpu.HBM)

    def pinned(array):
        return pltpu.with_memory_space_constraint(array, pltpu.HBM)

    def shaped(dims, kind):
        return jax.ShapeDtypeStruct(dims, kind)

    (
        normed,
        conv,
        mix,
        keep,
        after,
        kept_scale,
        valid,
        fresh_pick,
        cache_pick,
        group_kept,
        own_total,
    ) = pl.pallas_call(
        prepare_kernel,
        out_shape=[
            shaped((rows, model_width), BF16),
            shaped((rows, map_width), BF16),
            shaped((rows, lanes), F32),
            shaped((rows, lanes), F32),
            shaped((rows, lanes), F32),
            shaped((requests, heads), F32),
            shaped((rows, 128), F32),
            shaped((depth * requests, rows), BF16),
            shaped((depth * requests, depth * requests), BF16),
            pltpu.HBM((depth, requests, map_width), BF16),
            shaped((8, 128), jnp.int32),
        ],
        in_specs=[hbm] * 12,
        out_specs=[vmem] * 9 + [hbm, vmem],
        scratch_shapes=[
            pltpu.SMEM((requests,), jnp.int32),
            pltpu.SMEM((requests,), jnp.int32),
            pltpu.SMEM((requests,), jnp.int32),
            pltpu.VMEM((rows, model_width), BF16),
            pltpu.VMEM((1, model_width), F32),
            pltpu.VMEM(group_weight.shape, BF16),
            pltpu.VMEM(step_weight.shape[::-1], BF16),
            pltpu.VMEM((depth, requests, map_width), BF16),
            pltpu.VMEM(group_kernel.shape, BF16),
            pltpu.VMEM((1, map_width), BF16),
            pltpu.VMEM((1, heads), F32),
            pltpu.VMEM((1, heads), F32),
            pltpu.VMEM((depth, requests, map_width), BF16),
            pltpu.SemaphoreType.DMA((12,)),
            pltpu.SemaphoreType.DMA,
        ],
        compiler_params=pltpu.CompilerParams(vmem_limit_bytes=32 * 1024 * 1024),
    )(
        pinned(accepted),
        pinned(draft_lengths),
        pinned(live_flags),
        pinned(tokens.reshape(rows, model_width)),
        pinned(norm_gain.reshape(1, -1)),
        pinned(group_weight),
        pinned(step_weight.T),
        pinned(jnp.transpose(group_cache, (1, 0, 2))),
        pinned(group_kernel),
        pinned(group_offset.reshape(1, -1)),
        pinned(step_bias.reshape(1, -1)),
        pinned(decay_rate.reshape(1, -1)),
    )
    normed, value_offset = lax.optimization_barrier((normed, value_offset))
    inner_proj = jnp.einsum(
        "rd,dgi->gri", normed, in_weight, preferred_element_type=F32
    ).astype(BF16)

    cache_rows = jnp.transpose(value_cache, (1, 0, 2))
    fars = lax.axis_size("tensor") // 2
    block = (chunks, fars - 1, height, half // fars)
    out_rows, kept_state, totals = pl.pallas_call(
        layer_kernel,
        out_shape=[
            shaped((rows, model_width), BF16),
            shaped((requests, inner, state_size), BF16),
            shaped((1,), jnp.int32),
        ],
        in_specs=[smem] * 2 + [vmem] * 11 + [hbm] * 2,
        out_specs=[vmem, vmem, smem],
        scratch_shapes=[
            pltpu.VMEM((2, inner, half), BF16),
            pltpu.VMEM((requests, inner, state_size), BF16),
            pltpu.VMEM((chunks, height, half), BF16),
            pltpu.VMEM((chunks, height, half), BF16),
            pltpu.VMEM(block, BF16),
            pltpu.VMEM(block, BF16),
            pltpu.VMEM((chunks, height, half), F32),
            pltpu.VMEM((positions, lanes, inner), BF16),
            pltpu.VMEM((rows, map_width), BF16),
            pltpu.VMEM((rows, map_width), F32),
            pltpu.VMEM((rows, map_width), F32),
            pltpu.VMEM((rows, inner), F32),
            pltpu.VMEM((chunks, height, 128), F32),
            pltpu.VMEM((chunks, height, 128), F32),
            pltpu.VMEM((groups - 1, 8, 128), jnp.int32),
            pltpu.SemaphoreType.DMA((2,)),
            pltpu.SemaphoreType.DMA((chunks,)),
            pltpu.SemaphoreType.DMA((2, 1)),
            pltpu.SemaphoreType.DMA((2, chunks)),
            pltpu.SemaphoreType.DMA((2, chunks)),
            pltpu.SemaphoreType.DMA((2, chunks * (fars - 1))),
            pltpu.SemaphoreType.DMA((2, chunks * (fars - 1))),
            pltpu.SemaphoreType.DMA((2, chunks * fars)),
            pltpu.SemaphoreType.DMA((2, groups - 1)),
        ],
        compiler_params=pltpu.CompilerParams(
            collective_id=0, has_side_effects=True, vmem_limit_bytes=40 * 1024 * 1024
        ),
    )(
        kept_scale,
        skip_gain,
        inner_proj,
        conv,
        mix,
        keep,
        after,
        valid,
        cache_rows,
        value_kernel,
        value_offset.reshape(1, -1),
        out_gain.reshape(1, -1),
        own_total,
        pinned(out_weight),
        pinned(scan_state.reshape(requests, inner, state_size)),
    )
    out_rows, kept_state, value_kept = pl.pallas_call(
        finish_kernel,
        out_shape=[
            pltpu.HBM((rows, model_width), BF16),
            pltpu.HBM((requests, inner, state_size), BF16),
            pltpu.HBM((depth, requests, inner), BF16),
        ],
        in_specs=[vmem] * 6,
        out_specs=[hbm] * 3,
        scratch_shapes=[
            pltpu.VMEM((depth, requests, inner), BF16),
            pltpu.SemaphoreType.DMA((3,)),
        ],
        compiler_params=pltpu.CompilerParams(vmem_limit_bytes=16 * 1024 * 1024),
    )(out_rows, kept_state, inner_proj, cache_rows, fresh_pick, cache_pick)
    return (
        out_rows.reshape(requests, positions, model_width),
        kept_state.reshape(scan_state.shape),
        jnp.transpose(value_kept, (1, 0, 2)),
        jnp.transpose(group_kept, (1, 0, 2)),
        totals,
    )


def solution(mesh):
    placed = (
        P("dp", None, None),
        P(),
        P(None, None, "tensor"),
        P(None, "tensor"),
        P(None, "tensor"),
        P(None, "tensor"),
        P("tensor"),
        P(None, "tensor"),
        P("tensor"),
        P("tensor"),
        P("tensor"),
        P("tensor"),
        P("tensor"),
        P("tensor", None),
        P("dp", "tensor", None, None),
        P("dp", None, "tensor"),
        P("dp", None, "tensor"),
        P("dp"),
        P("dp"),
        P("dp"),
    )
    return jax.shard_map(
        local,
        mesh=mesh,
        in_specs=placed,
        out_specs=(
            P("dp", None, None),
            P("dp", "tensor", None, None),
            P("dp", None, "tensor"),
            P("dp", None, "tensor"),
            P(),
        ),
        check_vma=False,
    )
```

```python
import jax
import jax.numpy as jnp
from jax import lax
from jax.experimental import pallas as pl
from jax.experimental.pallas import tpu as pltpu
from jax.sharding import PartitionSpec as P

EPSILON = 1e-05
MESH = pl.DeviceIdType.MESH
F32 = jnp.float32
BF16 = jnp.bfloat16


def iota(shape, axis):
    return lax.broadcasted_iota(jnp.int32, shape, axis)


def dot(a, b):
    return jnp.dot(a, b, preferred_element_type=F32)


def dot_nt(a, b):
    return lax.dot_general(a, b, (((1,), (1,)), ((), ())), preferred_element_type=F32)


def dot_tn(a, b):
    return lax.dot_general(a, b, (((0,), (0,)), ((), ())), preferred_element_type=F32)


def dot_split(a, b):
    high = a.astype(BF16)
    low = (a - high.astype(F32)).astype(BF16)
    return dot(high, b) + dot(low, b)


def silu(v):
    return v * (1.0 / (1.0 + jnp.exp(-v)))


def spread_cache(cache, rows, positions, first):
    depth, requests, width = cache.shape
    flat = cache.reshape(depth * requests, width)
    row = iota((rows, depth * requests), 0)
    col = iota((rows, depth * requests), 1)
    place = row % positions - (positions - depth)
    chosen = (col == place * requests + first + row // positions) & (place >= 0)
    return dot(chosen.astype(BF16), flat)


def convolve(fresh, cached, kernel, offset, positions):
    rows, width = fresh.shape
    taps = kernel.shape[0]
    fresh = fresh.reshape(rows // positions, positions, width)
    cached = cached.reshape(rows // positions, positions, width)
    place = iota(fresh.shape, 1)
    total = offset[None] + kernel[taps - 1 : taps][None] * fresh
    for shift in range(1, taps):
        merged = jnp.where(place < positions - shift, fresh, cached)
        moved = pltpu.roll(merged, shift, axis=1)
        total = total + kernel[taps - 1 - shift : taps - shift][None] * moved
    return silu(total).reshape(rows, width)


def prepare_kernel(
    accepted_hbm,
    draft_hbm,
    live_hbm,
    tokens_hbm,
    gain_hbm,
    weight_hbm,
    step_weight_hbm,
    cache_hbm,
    kernel_hbm,
    offset_hbm,
    bias_hbm,
    rate_hbm,
    normed_ref,
    input_map_ref,
    output_map_ref,
    group_proj_ref,
    mix_ref,
    keep_ref,
    after_ref,
    scale_ref,
    valid_ref,
    fresh_pick_ref,
    cache_pick_ref,
    total_ref,
    accepted_ref,
    draft_ref,
    live_ref,
    tokens_ref,
    gain_ref,
    weight_ref,
    step_weight_ref,
    cache_ref,
    kernel_ref,
    offset_ref,
    bias_ref,
    rate_ref,
    map_send,
    map_recv,
    load_sems,
    map_sems,
):
    me = lax.axis_index("tensor")
    near = me % 2
    partner = me + 1 - 2 * near
    barrier = pltpu.get_barrier_semaphore()
    pl.semaphore_signal(barrier, inc=1, device_id={"tensor": partner}, device_id_type=MESH)
    sources = (gain_hbm, tokens_hbm, weight_hbm, step_weight_hbm, cache_hbm)
    sources += (kernel_hbm, offset_hbm, bias_hbm, rate_hbm, accepted_hbm, draft_hbm, live_hbm)
    targets = (gain_ref, tokens_ref, weight_ref, step_weight_ref, cache_ref)
    targets += (kernel_ref, offset_ref, bias_ref, rate_ref, accepted_ref, draft_ref, live_ref)
    loads = [
        pltpu.make_async_copy(source, target, load_sems.at[index])
        for index, (source, target) in enumerate(zip(sources, targets))
    ]
    for load in loads:
        load.start()
    rows, model_width = tokens_ref.shape
    requests = accepted_ref.shape[0]
    positions = rows // requests
    heads = bias_ref.shape[1]
    depth = cache_ref.shape[0]
    lanes = positions * heads
    step = 16 if rows % 16 == 0 else 8
    loads[0].wait()
    loads[1].wait()
    for start in range(0, rows, step):
        wide = tokens_ref[start : start + step].astype(F32)
        mean = jnp.sum(wide * wide, axis=1, keepdims=True) / model_width
        normed_ref[start : start + step] = (
            wide * lax.rsqrt(mean + EPSILON) * gain_ref[...]
        ).astype(BF16)
    for load in loads[2:]:
        load.wait()
    normed = normed_ref[...]
    group_proj = dot(normed, weight_ref[...]).astype(BF16)
    group_proj_ref[...] = group_proj

    cache = cache_ref[...]
    cached = spread_cache(cache, rows, positions, 0)
    conv = convolve(
        group_proj.astype(F32),
        cached,
        kernel_ref[...].astype(F32),
        offset_ref[...].astype(F32),
        positions,
    )
    map_send[...] = conv.astype(BF16)
    pl.semaphore_wait(barrier, 1)
    map_copy = pltpu.make_async_remote_copy(
        src_ref=map_send,
        dst_ref=map_recv,
        send_sem=map_sems.at[0],
        recv_sem=map_sems.at[1],
        device_id={"tensor": partner},
        device_id_type=MESH,
    )
    map_copy.start()
    step_raw = dot_nt(normed, step_weight_ref[...])

    counts = [accepted_ref[r] * live_ref[r] for r in range(requests)]
    total = counts[0]
    for count in counts[1:]:
        total = total + count
    total_ref[...] = jnp.full(total_ref.shape, total, jnp.int32)

    bias = jnp.concatenate([bias_ref[...]] * positions, axis=1)[None]
    rate = jnp.concatenate([rate_ref[...]] * positions, axis=1)[None]
    raw = jnp.concatenate([step_raw] * positions, axis=1).reshape(requests, positions, lanes)
    raw = raw + bias
    size = jnp.maximum(raw, 0.0) + jnp.log1p(jnp.exp(-jnp.abs(raw)))
    log_decay = -size * rate
    place = iota((requests, positions, lanes), 1)
    source = iota((requests, positions, lanes), 2) // heads
    after = log_decay
    shift = 1
    while shift < positions:
        after = after + jnp.where(place >= shift, pltpu.roll(after, shift, axis=1), 0.0)
        shift *= 2
    kept = jnp.stack([jnp.full((positions, lanes), count, jnp.int32) for count in counts])
    own = place == source
    after_source = jnp.sum(jnp.where(own, after, 0.0), axis=1, keepdims=True)
    size_source = jnp.sum(jnp.where(own, size, 0.0), axis=1, keepdims=True)
    causal = place >= source
    mix = jnp.where(causal, jnp.exp(jnp.where(causal, after - after_source, 0.0)), 0.0) * size_source
    kept_after = jnp.sum(jnp.where(place == kept - 1, after, 0.0), axis=1, keepdims=True)
    before = place < kept
    keep = jnp.where(before, jnp.exp(jnp.where(before, kept_after - after, 0.0)), 0.0) * size
    mix_ref[...] = mix.reshape(rows, lanes)
    keep_ref[...] = keep.reshape(rows, lanes)
    after_ref[...] = jnp.exp(after).reshape(rows, lanes)
    scale_ref[...] = jnp.exp(kept_after[:, 0, :heads])

    wide_lanes = valid_ref.shape[1]
    drafted = jnp.stack(
        [
            jnp.full((positions, wide_lanes), draft_ref[r] * (live_ref[r] == 1).astype(jnp.int32), jnp.int32)
            for r in range(requests)
        ]
    )
    valid = iota(drafted.shape, 1) < drafted
    valid_ref[...] = valid.astype(F32).reshape(rows, wide_lanes)

    def picks(width, position_of, request_of):
        shape = (requests, width)
        row = iota(shape, 0)
        count = jnp.zeros(shape, jnp.int32)
        for r in range(requests):
            count = jnp.where(row == r, counts[r], count)
        col = iota(shape, 1)
        return jnp.concatenate(
            [
                ((position_of(col) == count + t) & (request_of(col) == row)).astype(F32)
                for t in range(depth)
            ],
            axis=0,
        ).astype(BF16)

    fresh_pick = picks(rows, lambda col: col % positions + depth, lambda col: col // positions)
    cache_pick = picks(depth * requests, lambda col: col // requests, lambda col: col % requests)
    fresh_pick_ref[...] = fresh_pick
    cache_pick_ref[...] = cache_pick
    map_copy.wait_recv()
    mine, other = map_send[...].astype(F32), map_recv[...].astype(F32)
    input_map_ref[...] = jnp.where(near == 0, mine, other).astype(BF16)
    output_map_ref[...] = jnp.where(near == 0, other, mine).astype(BF16)
    map_copy.wait_send()


def layer_kernel(
    scale_ref,
    skip_ref,
    inner_ref,
    input_map,
    output_map,
    mix_ref,
    keep_ref,
    after_ref,
    valid_ref,
    cache_ref,
    kernel_ref,
    offset_ref,
    gain_ref,
    count_ref,
    weight_hbm,
    state_hbm,
    out_buf,
    kept_buf,
    total_ref,
    weight_buf,
    state_buf,
    y_send,
    y_recv,
    n_send,
    n_recv,
    f_send,
    f_recv,
    acc_buf,
    place_buf,
    weighted_buf,
    sq_send,
    sq_recv,
    count_recv,
    weight_sem,
    state_sem,
    sq_sems,
    y_sems,
    n_sems,
    f_sems,
    o_sems,
    p_sems,
    count_sems,
):
    chunks, height, half = y_send.shape
    rows, inner = inner_ref.shape[1:]
    requests = state_buf.shape[0]
    positions = rows // requests
    lanes = mix_ref.shape[1]
    heads = lanes // positions
    head_dim = inner // heads
    per_chunk = requests // chunks
    depth = cache_ref.shape[0]

    members = lax.axis_size("tensor")
    fars = members // 2
    width = half // fars
    me = lax.axis_index("tensor")
    far, near = me // 2, me % 2
    partner = far * 2 + (1 - near)

    team = fars // 2
    wing, seat = far // team, far % team
    mate = (1 - wing) * team + seat

    def peer_at(step):
        return wing * team + lax.rem(seat + 1 + step, team)

    def peer_of(step):
        return wing * team + lax.rem(seat - 1 - step + 2 * team, team)

    def across(place):
        return lax.rem(place + team, fars)

    def device(place):
        return place * 2 + near

    groups = lax.axis_size("dp")
    group = lax.axis_index("dp")

    def cols(start, width):
        return pl.ds(pl.multiple_of(start, width), width)

    weight_loads = [
        pltpu.make_async_copy(
            weight_hbm.at[:, cols(block * half, half)],
            weight_buf.at[slot],
            weight_sem.at[slot],
        )
        for slot, block in enumerate((1 - near, near))
    ]
    state_loads = [
        pltpu.make_async_copy(
            state_hbm.at[pl.ds(c * per_chunk, per_chunk)],
            state_buf.at[pl.ds(c * per_chunk, per_chunk)],
            state_sem.at[c],
        )
        for c in range(chunks)
    ]
    state_loads[0].start()
    weight_loads[0].start()
    weight_loads[1].start()
    for load in state_loads[1:]:
        load.start()

    barrier = pltpu.get_barrier_semaphore()
    pl.semaphore_signal(barrier, inc=1, device_id={"tensor": partner}, device_id_type=MESH)

    for place in [mate] + [peer_at(step) for step in range(team - 1)]:
        pl.semaphore_signal(
            barrier, inc=1, device_id={"tensor": device(place)}, device_id_type=MESH
        )
    for hop in range(groups - 1):
        pl.semaphore_signal(
            barrier,
            inc=1,
            device_id={"dp": lax.rem(group + 1 + hop, groups)},
            device_id_type=MESH,
        )
    def remote(source, target, sems, index, device):
        return pltpu.make_async_remote_copy(
            src_ref=source,
            dst_ref=target,
            send_sem=sems.at[0, index],
            recv_sem=sems.at[1, index],
            device_id={"tensor": device},
            device_id_type=MESH,
        )

    shape = (lanes, inner)
    target_head = iota(shape, 1) // head_dim
    lane_row = iota(shape, 0)
    for j in range(positions):
        place_buf[j] = (lane_row == target_head + j * heads).astype(F32).astype(BF16)
    to_heads = place_buf[0]

    lane_head = iota((1, inner), 1) // head_dim
    skip = jnp.zeros((1, inner), F32)
    for h in range(heads):
        skip = jnp.where(lane_head == h, skip_ref[h], skip)

    cache = cache_ref[...]
    kernel = kernel_ref[...].astype(F32)
    offset = offset_ref[...].astype(F32)

    def values_of(c):
        span = slice(c * height, (c + 1) * height)
        cached = spread_cache(cache, height, positions, c * per_chunk)
        return convolve(inner_ref[1, span].astype(F32), cached, kernel, offset, positions)

    def front(c):
        span = slice(c * height, (c + 1) * height)
        values = values_of(c)
        gate = silu(inner_ref[0, span].astype(F32))
        align = dot_nt(output_map[span], input_map[span])
        square = (height, height)
        same = iota(square, 0) // positions == iota(square, 1) // positions
        fold = (height, lanes)
        folded = (iota(fold, 0) % positions == iota(fold, 1) // heads).astype(F32).astype(BF16)
        mix = (mix_ref[span] * dot_split(jnp.where(same, align, 0.0), folded)).astype(BF16)
        values3 = values.reshape(per_chunk, positions, inner)
        head = skip * values
        for j in range(positions):
            spread = jnp.broadcast_to(values3[:, j : j + 1], values3.shape).reshape(height, inner)
            head = head + dot(mix, place_buf[j]) * spread
        state_loads[c].wait()
        outputs = output_map[span].astype(F32)
        carried = jnp.concatenate(
            [
                dot_nt(
                    outputs[(r - c * per_chunk) * positions :][:positions].astype(BF16), state_buf[r]
                )
                for r in range(c * per_chunk, (c + 1) * per_chunk)
            ],
            axis=0,
        )
        head = head + carried * dot_split(after_ref[span], to_heads)
        gated = head * gate
        squares = jnp.sum(gated * gated, axis=1, keepdims=True)
        sq_send[c] = jnp.broadcast_to(squares, sq_send.shape[1:])
        if c == 0:
            pl.semaphore_wait(barrier, fars // 2 + groups)
        sq_copies[c].start()
        weighted_buf[span] = values * dot_split(keep_ref[span], to_heads)
        return (gated * gain_ref[...]).astype(BF16)

    sq_copies = [
        remote(sq_send.at[c], sq_recv.at[c], sq_sems, c, partner) for c in range(chunks)
    ]
    y_copies = [remote(y_send.at[c], y_recv.at[c], y_sems, c, partner) for c in range(chunks)]
    n_copies = [
        [
            remote(
                n_send.at[c, step],
                n_recv.at[c, step],
                n_sems,
                c * (team - 1) + step,
                device(peer_at(step)),
            )
            for step in range(team - 1)
        ]
        for c in range(chunks)
    ]
    f_copies = [
        remote(f_send.at[c], f_recv.at[c], f_sems, c, device(mate)) for c in range(chunks)
    ]

    def region(c, plane, owner):
        return out_buf.at[pl.ds(c * height, height), cols(plane * half + owner * width, width)]

    def owned(c, owner, sems, index, device, plane=near):
        return remote(region(c, plane, owner), region(c, plane, owner), sems, index, device)

    def send_partial(c):
        rows_in = front(c)
        if c == 0:
            weight_loads[0].wait()
        y_send[c] = dot(rows_in, weight_buf[0]).astype(BF16)
        y_copies[c].start()
        if c == 0:
            weight_loads[1].wait()
        acc_buf[c] = dot(rows_in, weight_buf[1])

    def pair_sum(c):
        span = slice(c * height, (c + 1) * height)
        sq_copies[c].wait_recv()
        total = (sq_send[c] + sq_recv[c])[:, :1] / (2 * inner)
        scale = lax.rsqrt(total + EPSILON) * valid_ref[span, :1]
        y_copies[c].wait_recv()
        acc_buf[c] = (acc_buf[c] + y_recv[c].astype(F32)) * scale

        for step in range(team - 1):
            place = peer_at(step)
            n_send[c, step, 0] = acc_buf[c, :, cols(place * width, width)].astype(BF16)
            n_send[c, step, 1] = acc_buf[c, :, cols(across(place) * width, width)].astype(BF16)
            n_copies[c][step].start()

    def team_sum(c):
        own = acc_buf[c, :, cols(far * width, width)]
        other = acc_buf[c, :, cols(mate * width, width)]
        for step in range(team - 1):
            n_copies[c][step].wait_recv()
            own = own + n_recv[c, step, 0].astype(F32)
            other = other + n_recv[c, step, 1].astype(F32)
        f_send[c] = other.astype(BF16)
        f_copies[c].start()
        acc_buf[c, :, cols(far * width, width)] = own

    sent = []

    def send(copy):
        copy.start()
        sent.append(copy)

    per_o, per_p = 2 * team - 1, 2 * team

    def send_final(c):
        f_copies[c].wait_recv()
        total = acc_buf[c, :, cols(far * width, width)] + f_recv[c].astype(F32)
        span = pl.ds(c * height, height)
        out_buf[span, cols(near * half + far * width, width)] = total.astype(BF16)
        send(owned(c, far, o_sems, c * per_o, device(mate)))
        for step in range(team - 1):
            send(owned(c, far, o_sems, c * per_o + 1 + step, device(peer_at(step))))
        send(owned(c, far, p_sems, c * per_p, partner))

    def forward(c):
        owned(c, mate, o_sems, c * per_o, partner).wait_recv()
        for step in range(team - 1):
            send(owned(c, mate, o_sems, c * per_o + team + step, device(peer_at(step))))
        send(owned(c, mate, p_sems, c * per_p + 1, partner))
        for step in range(team - 1):
            place = peer_of(step)
            owned(c, place, o_sems, c * per_o + 1 + step, partner).wait_recv()
            send(owned(c, place, p_sems, c * per_p + 2 + step, partner))

    def forward_last(c):
        for step in range(team - 1):
            place = across(peer_of(step))
            owned(c, place, o_sems, c * per_o + team + step, partner).wait_recv()
            send(owned(c, place, p_sems, c * per_p + team + 1 + step, partner))

    def complete(c):
        places = [far, mate]
        places += [peer_of(step) for step in range(team - 1)]
        places += [across(peer_of(step)) for step in range(team - 1)]
        for index, place in enumerate(places):
            owned(c, place, p_sems, c * per_p + index, partner, 1 - near).wait_recv()

    def keep_state(c):
        for r in range(c * per_chunk, (c + 1) * per_chunk):
            span = slice(r * positions, (r + 1) * positions)
            added = dot_tn(weighted_buf[span].astype(BF16), input_map[span])
            for h in range(heads):
                block = slice(h * head_dim, (h + 1) * head_dim)
                kept_buf[r, block] = (
                    scale_ref[r, h] * state_buf[r, block].astype(F32) + added[block]
                ).astype(BF16)

    plan = (
        (send_partial, 0, 2.8),
        (pair_sum, 5.1, 2.8),
        (team_sum, 8.8, 2.8),
        (send_final, 11.8, 2.8),
        (forward, 14.8, 2.8),
        (forward_last, 17.8, 2.8),
        (keep_state, 18, 1.4),
        (complete, 40.0, 1.0),
    )
    events = [
        (first + spacing * c, index, c)
        for index, (_, first, spacing) in enumerate(plan)
        for c in range(chunks)
    ]
    count_copies = []
    for _, index, c in sorted(events):
        plan[index][0](c)
        if plan[index][0] is send_partial and c == 0:
            for hop in range(groups - 1):
                copy = pltpu.make_async_remote_copy(
                    src_ref=count_ref,
                    dst_ref=count_recv.at[hop],
                    send_sem=count_sems.at[0, hop],
                    recv_sem=count_sems.at[1, hop],
                    device_id={"dp": lax.rem(group + 1 + hop, groups)},
                    device_id_type=MESH,
                )
                copy.start()
                count_copies.append(copy)

    count = count_ref[...]
    for hop in range(groups - 1):
        count_copies[hop].wait_recv()
        count = count + count_recv[hop]
    total_ref[0] = count[0, 0]

    for copy in sq_copies + y_copies + sum(n_copies, []) + f_copies + sent + count_copies:
        copy.wait_send()


def finish_kernel(
    rows_ref,
    kept_ref,
    inner_ref,
    cache_ref,
    group_proj_ref,
    group_cache_ref,
    fresh_pick_ref,
    cache_pick_ref,
    rows_hbm,
    kept_hbm,
    value_kept_hbm,
    group_kept_hbm,
    value_kept_ref,
    group_kept_ref,
    sems,
):
    copies = [
        pltpu.make_async_copy(rows_ref, rows_hbm, sems.at[0]),
        pltpu.make_async_copy(kept_ref, kept_hbm, sems.at[1]),
        pltpu.make_async_copy(value_kept_ref, value_kept_hbm, sems.at[2]),
        pltpu.make_async_copy(group_kept_ref, group_kept_hbm, sems.at[3]),
    ]
    copies[0].start()
    copies[1].start()
    def kept(fresh, cache, target, copy):
        flat = cache.reshape(-1, cache.shape[2])
        rows = dot(fresh_pick_ref[...], fresh) + dot(cache_pick_ref[...], flat)
        target[...] = rows.reshape(target.shape).astype(BF16)
        copy.start()

    kept(inner_ref[1], cache_ref[...], value_kept_ref, copies[2])
    kept(group_proj_ref[...], group_cache_ref[...], group_kept_ref, copies[3])
    for copy in copies:
        copy.wait()


def local(
    tokens,
    norm_gain,
    in_weight,
    group_weight,
    step_weight,
    value_kernel,
    value_offset,
    group_kernel,
    group_offset,
    step_bias,
    decay_rate,
    skip_gain,
    out_gain,
    out_weight,
    scan_state,
    value_cache,
    group_cache,
    accepted,
    draft_lengths,
    live_flags,
):
    requests, positions, model_width = tokens.shape
    rows = requests * positions
    heads, head_dim, state_size = scan_state.shape[1:]
    inner = heads * head_dim
    map_width = group_weight.shape[1]
    depth = value_cache.shape[1]
    lanes = positions * heads
    groups = lax.axis_size("dp")
    chunks = next(c for c in (6, 4, 3, 2, 1) if requests % c == 0 and (rows // c) % 16 == 0)
    height = rows // chunks
    half = model_width // 2
    vmem = pl.BlockSpec(memory_space=pltpu.VMEM)
    smem = pl.BlockSpec(memory_space=pltpu.SMEM)
    hbm = pl.BlockSpec(memory_space=pltpu.HBM)

    def pinned(array):
        return pltpu.with_memory_space_constraint(array, pltpu.HBM)

    def shaped(dims, kind):
        return jax.ShapeDtypeStruct(dims, kind)

    (
        normed,
        input_map,
        output_map,
        group_proj,
        mix,
        keep,
        after,
        kept_scale,
        valid,
        fresh_pick,
        cache_pick,
        own_total,
    ) = pl.pallas_call(
        prepare_kernel,
        out_shape=[
            shaped((rows, model_width), BF16),
            shaped((rows, map_width), BF16),
            shaped((rows, map_width), BF16),
            shaped((rows, map_width), BF16),
            shaped((rows, lanes), F32),
            shaped((rows, lanes), F32),
            shaped((rows, lanes), F32),
            shaped((requests, heads), F32),
            shaped((rows, 128), F32),
            shaped((depth * requests, rows), BF16),
            shaped((depth * requests, depth * requests), BF16),
            shaped((8, 128), jnp.int32),
        ],
        in_specs=[hbm] * 12,
        out_specs=[vmem] * 12,
        scratch_shapes=[
            pltpu.SMEM((requests,), jnp.int32),
            pltpu.SMEM((requests,), jnp.int32),
            pltpu.SMEM((requests,), jnp.int32),
            pltpu.VMEM((rows, model_width), BF16),
            pltpu.VMEM((1, model_width), F32),
            pltpu.VMEM(group_weight.shape, BF16),
            pltpu.VMEM(step_weight.shape[::-1], BF16),
            pltpu.VMEM((depth, requests, map_width), BF16),
            pltpu.VMEM(group_kernel.shape, BF16),
            pltpu.VMEM((1, map_width), BF16),
            pltpu.VMEM((1, heads), F32),
            pltpu.VMEM((1, heads), F32),
            pltpu.VMEM((rows, map_width), BF16),
            pltpu.VMEM((rows, map_width), BF16),
            pltpu.SemaphoreType.DMA((12,)),
            pltpu.SemaphoreType.DMA((2,)),
        ],
        compiler_params=pltpu.CompilerParams(
            collective_id=1, has_side_effects=True, vmem_limit_bytes=32 * 1024 * 1024
        ),
    )(
        pinned(accepted),
        pinned(draft_lengths),
        pinned(live_flags),
        pinned(tokens.reshape(rows, model_width)),
        pinned(norm_gain.reshape(1, -1)),
        pinned(group_weight),
        pinned(step_weight.T),
        pinned(jnp.transpose(group_cache, (1, 0, 2))),
        pinned(group_kernel),
        pinned(group_offset.reshape(1, -1)),
        pinned(step_bias.reshape(1, -1)),
        pinned(decay_rate.reshape(1, -1)),
    )
    normed, value_offset = lax.optimization_barrier((normed, value_offset))
    inner_proj = jnp.einsum(
        "rd,dgi->gri", normed, in_weight, preferred_element_type=F32
    ).astype(BF16)

    cache_rows = jnp.transpose(value_cache, (1, 0, 2))
    fars = lax.axis_size("tensor") // 2
    team = fars // 2
    width = half // fars
    out_rows, kept_state, totals = pl.pallas_call(
        layer_kernel,
        out_shape=[
            shaped((rows, model_width), BF16),
            shaped((requests, inner, state_size), BF16),
            shaped((1,), jnp.int32),
        ],
        in_specs=[smem] * 2 + [vmem] * 12 + [hbm] * 2,
        out_specs=[vmem, vmem, smem],
        scratch_shapes=[
            pltpu.VMEM((2, inner, half), BF16),
            pltpu.VMEM((requests, inner, state_size), BF16),
            pltpu.VMEM((chunks, height, half), BF16),
            pltpu.VMEM((chunks, height, half), BF16),
            pltpu.VMEM((chunks, team - 1, 2, height, width), BF16),
            pltpu.VMEM((chunks, team - 1, 2, height, width), BF16),
            pltpu.VMEM((chunks, height, width), BF16),
            pltpu.VMEM((chunks, height, width), BF16),
            pltpu.VMEM((chunks, height, half), F32),
            pltpu.VMEM((positions, lanes, inner), BF16),
            pltpu.VMEM((rows, inner), F32),
            pltpu.VMEM((chunks, height, 128), F32),
            pltpu.VMEM((chunks, height, 128), F32),
            pltpu.VMEM((groups - 1, 8, 128), jnp.int32),
            pltpu.SemaphoreType.DMA((2,)),
            pltpu.SemaphoreType.DMA((chunks,)),
            pltpu.SemaphoreType.DMA((2, chunks)),
            pltpu.SemaphoreType.DMA((2, chunks)),
            pltpu.SemaphoreType.DMA((2, chunks * (team - 1))),
            pltpu.SemaphoreType.DMA((2, chunks)),
            pltpu.SemaphoreType.DMA((2, chunks * (2 * team - 1))),
            pltpu.SemaphoreType.DMA((2, chunks * 2 * team)),
            pltpu.SemaphoreType.DMA((2, groups - 1)),
        ],
        compiler_params=pltpu.CompilerParams(
            collective_id=0, has_side_effects=True, vmem_limit_bytes=40 * 1024 * 1024
        ),
    )(
        kept_scale,
        skip_gain,
        inner_proj,
        input_map,
        output_map,
        mix,
        keep,
        after,
        valid,
        cache_rows,
        value_kernel,
        value_offset.reshape(1, -1),
        out_gain.reshape(1, -1),
        own_total,
        pinned(out_weight),
        pinned(scan_state.reshape(requests, inner, state_size)),
    )
    group_rows = jnp.transpose(group_cache, (1, 0, 2))
    out_rows, kept_state, value_kept, group_kept = pl.pallas_call(
        finish_kernel,
        out_shape=[
            pltpu.HBM((rows, model_width), BF16),
            pltpu.HBM((requests, inner, state_size), BF16),
            pltpu.HBM((depth, requests, inner), BF16),
            pltpu.HBM((depth, requests, map_width), BF16),
        ],
        in_specs=[vmem] * 8,
        out_specs=[hbm] * 4,
        scratch_shapes=[
            pltpu.VMEM((depth, requests, inner), BF16),
            pltpu.VMEM((depth, requests, map_width), BF16),
            pltpu.SemaphoreType.DMA((4,)),
        ],
        compiler_params=pltpu.CompilerParams(vmem_limit_bytes=16 * 1024 * 1024),
    )(
        out_rows,
        kept_state,
        inner_proj,
        cache_rows,
        group_proj,
        group_rows,
        fresh_pick,
        cache_pick,
    )
    return (
        out_rows.reshape(requests, positions, model_width),
        kept_state.reshape(scan_state.shape),
        jnp.transpose(value_kept, (1, 0, 2)),
        jnp.transpose(group_kept, (1, 0, 2)),
        totals,
    )


def solution(mesh):
    placed = (
        P("dp", None, None),
        P(),
        P(None, None, "tensor"),
        P(None, "tensor"),
        P(None, "tensor"),
        P(None, "tensor"),
        P("tensor"),
        P(None, "tensor"),
        P("tensor"),
        P("tensor"),
        P("tensor"),
        P("tensor"),
        P("tensor"),
        P("tensor", None),
        P("dp", "tensor", None, None),
        P("dp", None, "tensor"),
        P("dp", None, "tensor"),
        P("dp"),
        P("dp"),
        P("dp"),
    )
    return jax.shard_map(
        local,
        mesh=mesh,
        in_specs=placed,
        out_specs=(
            P("dp", None, None),
            P("dp", "tensor", None, None),
            P("dp", None, "tensor"),
            P("dp", None, "tensor"),
            P(),
        ),
        check_vma=False,
    )
```

```python
import jax
import jax.numpy as jnp
from jax import lax
from jax.experimental import pallas as pl
from jax.experimental.pallas import tpu as pltpu
from jax.sharding import PartitionSpec as P

EPSILON = 1e-05
MESH = pl.DeviceIdType.MESH
F32 = jnp.float32
BF16 = jnp.bfloat16


def iota(shape, axis):
    return lax.broadcasted_iota(jnp.int32, shape, axis)


def dot(a, b):
    return jnp.dot(a, b, preferred_element_type=F32)


def dot_nt(a, b):
    return lax.dot_general(a, b, (((1,), (1,)), ((), ())), preferred_element_type=F32)


def dot_tn(a, b):
    return lax.dot_general(a, b, (((0,), (0,)), ((), ())), preferred_element_type=F32)


def dot_split(a, b):
    high = a.astype(BF16)
    low = (a - high.astype(F32)).astype(BF16)
    return dot(high, b) + dot(low, b)


def silu(v):
    return v * (1.0 / (1.0 + jnp.exp(-v)))


def spread_cache(cache, rows, positions, first):
    depth, requests, width = cache.shape
    flat = cache.reshape(depth * requests, width)
    row = iota((rows, depth * requests), 0)
    col = iota((rows, depth * requests), 1)
    place = row % positions - (positions - depth)
    chosen = (col == place * requests + first + row // positions) & (place >= 0)
    return dot(chosen.astype(BF16), flat)


def convolve(fresh, cached, kernel, offset, positions):
    rows, width = fresh.shape
    taps = kernel.shape[0]
    fresh = fresh.reshape(rows // positions, positions, width)
    cached = cached.reshape(rows // positions, positions, width)
    place = iota(fresh.shape, 1)
    total = offset[None] + kernel[taps - 1 : taps][None] * fresh
    for shift in range(1, taps):
        merged = jnp.where(place < positions - shift, fresh, cached)
        moved = pltpu.roll(merged, shift, axis=1)
        total = total + kernel[taps - 1 - shift : taps - shift][None] * moved
    return silu(total).reshape(rows, width)


def prepare_kernel(
    accepted_hbm,
    draft_hbm,
    live_hbm,
    tokens_hbm,
    gain_hbm,
    weight_hbm,
    step_weight_hbm,
    cache_hbm,
    kernel_hbm,
    offset_hbm,
    bias_hbm,
    rate_hbm,
    in_weight_hbm,
    out_weight_hbm,
    normed_ref,
    input_map_ref,
    output_map_ref,
    group_proj_ref,
    mix_ref,
    keep_ref,
    after_ref,
    scale_ref,
    valid_ref,
    fresh_pick_ref,
    cache_pick_ref,
    total_ref,
    in_weight_ref,
    out_weight_ref,
    accepted_ref,
    draft_ref,
    live_ref,
    tokens_ref,
    gain_ref,
    weight_ref,
    step_weight_ref,
    cache_ref,
    kernel_ref,
    offset_ref,
    bias_ref,
    rate_ref,
    map_send,
    map_recv,
    load_sems,
    map_sems,
    weight_sem,
):
    me = lax.axis_index("tensor")
    near = me % 2
    partner = me + 1 - 2 * near
    barrier = pltpu.get_barrier_semaphore()
    pl.semaphore_signal(barrier, inc=1, device_id={"tensor": partner}, device_id_type=MESH)
    sources = (gain_hbm, tokens_hbm, weight_hbm, step_weight_hbm, cache_hbm)
    sources += (kernel_hbm, offset_hbm, bias_hbm, rate_hbm, accepted_hbm, draft_hbm, live_hbm)
    targets = (gain_ref, tokens_ref, weight_ref, step_weight_ref, cache_ref)
    targets += (kernel_ref, offset_ref, bias_ref, rate_ref, accepted_ref, draft_ref, live_ref)
    loads = [
        pltpu.make_async_copy(source, target, load_sems.at[index])
        for index, (source, target) in enumerate(zip(sources, targets))
    ]
    for load in loads:
        load.start()
    rows, model_width = tokens_ref.shape
    requests = accepted_ref.shape[0]
    positions = rows // requests
    heads = bias_ref.shape[1]
    depth = cache_ref.shape[0]
    lanes = positions * heads
    step = 16 if rows % 16 == 0 else 8
    loads[0].wait()
    loads[1].wait()
    weight_loads = [
        pltpu.make_async_copy(in_weight_hbm, in_weight_ref, weight_sem.at[0]),
        pltpu.make_async_copy(out_weight_hbm, out_weight_ref, weight_sem.at[1]),
    ]
    for load in weight_loads:
        load.start()
    for start in range(0, rows, step):
        wide = tokens_ref[start : start + step].astype(F32)
        mean = jnp.sum(wide * wide, axis=1, keepdims=True) / model_width
        normed_ref[start : start + step] = (
            wide * lax.rsqrt(mean + EPSILON) * gain_ref[...]
        ).astype(BF16)
    for load in loads[2:]:
        load.wait()
    normed = normed_ref[...]
    group_proj = dot(normed, weight_ref[...]).astype(BF16)
    group_proj_ref[...] = group_proj

    cache = cache_ref[...]
    cached = spread_cache(cache, rows, positions, 0)
    conv = convolve(
        group_proj.astype(F32),
        cached,
        kernel_ref[...].astype(F32),
        offset_ref[...].astype(F32),
        positions,
    )
    map_send[...] = conv.astype(BF16)
    pl.semaphore_wait(barrier, 1)
    map_copy = pltpu.make_async_remote_copy(
        src_ref=map_send,
        dst_ref=map_recv,
        send_sem=map_sems.at[0],
        recv_sem=map_sems.at[1],
        device_id={"tensor": partner},
        device_id_type=MESH,
    )
    map_copy.start()
    step_raw = dot_nt(normed, step_weight_ref[...])

    counts = [accepted_ref[r] * live_ref[r] for r in range(requests)]
    total = counts[0]
    for count in counts[1:]:
        total = total + count
    total_ref[...] = jnp.full(total_ref.shape, total, jnp.int32)

    bias = jnp.concatenate([bias_ref[...]] * positions, axis=1)[None]
    rate = jnp.concatenate([rate_ref[...]] * positions, axis=1)[None]
    raw = jnp.concatenate([step_raw] * positions, axis=1).reshape(requests, positions, lanes)
    raw = raw + bias
    size = jnp.maximum(raw, 0.0) + jnp.log1p(jnp.exp(-jnp.abs(raw)))
    log_decay = -size * rate
    place = iota((requests, positions, lanes), 1)
    source = iota((requests, positions, lanes), 2) // heads
    after = log_decay
    shift = 1
    while shift < positions:
        after = after + jnp.where(place >= shift, pltpu.roll(after, shift, axis=1), 0.0)
        shift *= 2
    kept = jnp.stack([jnp.full((positions, lanes), count, jnp.int32) for count in counts])
    own = place == source
    after_source = jnp.sum(jnp.where(own, after, 0.0), axis=1, keepdims=True)
    size_source = jnp.sum(jnp.where(own, size, 0.0), axis=1, keepdims=True)
    causal = place >= source
    mix = jnp.where(causal, jnp.exp(jnp.where(causal, after - after_source, 0.0)), 0.0) * size_source
    kept_after = jnp.sum(jnp.where(place == kept - 1, after, 0.0), axis=1, keepdims=True)
    before = place < kept
    keep = jnp.where(before, jnp.exp(jnp.where(before, kept_after - after, 0.0)), 0.0) * size
    mix_ref[...] = mix.reshape(rows, lanes)
    keep_ref[...] = keep.reshape(rows, lanes)
    after_ref[...] = jnp.exp(after).reshape(rows, lanes)
    scale_ref[...] = jnp.exp(kept_after[:, 0, :heads])

    wide_lanes = valid_ref.shape[1]
    drafted = jnp.stack(
        [
            jnp.full((positions, wide_lanes), draft_ref[r] * (live_ref[r] == 1).astype(jnp.int32), jnp.int32)
            for r in range(requests)
        ]
    )
    valid = iota(drafted.shape, 1) < drafted
    valid_ref[...] = valid.astype(F32).reshape(rows, wide_lanes)

    def picks(width, position_of, request_of):
        shape = (requests, width)
        row = iota(shape, 0)
        count = jnp.zeros(shape, jnp.int32)
        for r in range(requests):
            count = jnp.where(row == r, counts[r], count)
        col = iota(shape, 1)
        return jnp.concatenate(
            [
                ((position_of(col) == count + t) & (request_of(col) == row)).astype(F32)
                for t in range(depth)
            ],
            axis=0,
        ).astype(BF16)

    fresh_pick = picks(rows, lambda col: col % positions + depth, lambda col: col // positions)
    cache_pick = picks(depth * requests, lambda col: col // requests, lambda col: col % requests)
    fresh_pick_ref[...] = fresh_pick
    cache_pick_ref[...] = cache_pick
    map_copy.wait_recv()
    mine, other = map_send[...].astype(F32), map_recv[...].astype(F32)
    input_map_ref[...] = jnp.where(near == 0, mine, other).astype(BF16)
    output_map_ref[...] = jnp.where(near == 0, other, mine).astype(BF16)
    map_copy.wait_send()
    for load in weight_loads:
        load.wait()


def across_first_chunks(chunks):
    return {1: 0} if chunks >= 6 else {}


def layer_kernel(
    scale_ref,
    skip_ref,
    inner_ref,
    input_map,
    output_map,
    mix_ref,
    keep_ref,
    after_ref,
    valid_ref,
    cache_ref,
    kernel_ref,
    offset_ref,
    gain_ref,
    count_ref,
    weight_ref,
    state_hbm,
    out_buf,
    kept_buf,
    total_ref,
    state_buf,
    y_send,
    y_recv,
    n_send,
    n_recv,
    f_send,
    f_recv,
    acc_buf,
    zn_send,
    zn_recv,
    zf_send,
    zf_recv,
    zacc_buf,
    place_buf,
    weighted_buf,
    sq_send,
    sq_recv,
    count_recv,
    state_sem,
    sq_sems,
    y_sems,
    n_sems,
    f_sems,
    o_sems,
    p_sems,
    count_sems,
):
    chunks, height, half = y_send.shape
    rows, inner = inner_ref.shape[1:]
    requests = state_buf.shape[0]
    positions = rows // requests
    lanes = mix_ref.shape[1]
    heads = lanes // positions
    head_dim = inner // heads
    per_chunk = requests // chunks
    across_first = across_first_chunks(chunks)
    depth = cache_ref.shape[0]

    members = lax.axis_size("tensor")
    fars = members // 2
    width = half // fars
    me = lax.axis_index("tensor")
    far, near = me // 2, me % 2
    partner = far * 2 + (1 - near)

    team = fars // 2
    wing, seat = far // team, far % team
    mate = (1 - wing) * team + seat

    def peer_at(step):
        return wing * team + lax.rem(seat + 1 + step, team)

    def peer_of(step):
        return wing * team + lax.rem(seat - 1 - step + 2 * team, team)

    def across(place):
        return lax.rem(place + team, fars)

    def device(place):
        return place * 2 + near

    groups = lax.axis_size("dp")
    group = lax.axis_index("dp")

    def cols(start, width):
        return pl.ds(pl.multiple_of(start, width), width)

    state_loads = [
        pltpu.make_async_copy(
            state_hbm.at[pl.ds(c * per_chunk, per_chunk)],
            state_buf.at[pl.ds(c * per_chunk, per_chunk)],
            state_sem.at[c],
        )
        for c in range(chunks)
    ]
    state_loads[0].start()
    for load in state_loads[1:]:
        load.start()

    barrier = pltpu.get_barrier_semaphore()
    pl.semaphore_signal(barrier, inc=1, device_id={"tensor": partner}, device_id_type=MESH)

    for place in [mate] + [peer_at(step) for step in range(team - 1)]:
        pl.semaphore_signal(
            barrier, inc=1, device_id={"tensor": device(place)}, device_id_type=MESH
        )
    for hop in range(groups - 1):
        pl.semaphore_signal(
            barrier,
            inc=1,
            device_id={"dp": lax.rem(group + 1 + hop, groups)},
            device_id_type=MESH,
        )
    def remote(source, target, sems, index, device):
        return pltpu.make_async_remote_copy(
            src_ref=source,
            dst_ref=target,
            send_sem=sems.at[0, index],
            recv_sem=sems.at[1, index],
            device_id={"tensor": device},
            device_id_type=MESH,
        )

    shape = (lanes, inner)
    target_head = iota(shape, 1) // head_dim
    lane_row = iota(shape, 0)
    for j in range(positions):
        place_buf[j] = (lane_row == target_head + j * heads).astype(F32).astype(BF16)
    to_heads = place_buf[0]

    lane_head = iota((1, inner), 1) // head_dim
    skip = jnp.zeros((1, inner), F32)
    for h in range(heads):
        skip = jnp.where(lane_head == h, skip_ref[h], skip)

    cache = cache_ref[...]
    kernel = kernel_ref[...].astype(F32)
    offset = offset_ref[...].astype(F32)

    def values_of(c):
        span = slice(c * height, (c + 1) * height)
        cached = spread_cache(cache, height, positions, c * per_chunk)
        return convolve(inner_ref[1, span].astype(F32), cached, kernel, offset, positions)

    def front(c):
        span = slice(c * height, (c + 1) * height)
        values = values_of(c)
        gate = silu(inner_ref[0, span].astype(F32))
        align = dot_nt(output_map[span], input_map[span])
        square = (height, height)
        same = iota(square, 0) // positions == iota(square, 1) // positions
        fold = (height, lanes)
        folded = (iota(fold, 0) % positions == iota(fold, 1) // heads).astype(F32).astype(BF16)
        mix = (mix_ref[span] * dot_split(jnp.where(same, align, 0.0), folded)).astype(BF16)
        values3 = values.reshape(per_chunk, positions, inner)
        head = skip * values
        for j in range(positions):
            spread = jnp.broadcast_to(values3[:, j : j + 1], values3.shape).reshape(height, inner)
            head = head + dot(mix, place_buf[j]) * spread
        state_loads[c].wait()
        outputs = output_map[span].astype(F32)
        carried = jnp.concatenate(
            [
                dot_nt(
                    outputs[(r - c * per_chunk) * positions :][:positions].astype(BF16), state_buf[r]
                )
                for r in range(c * per_chunk, (c + 1) * per_chunk)
            ],
            axis=0,
        )
        head = head + carried * dot_split(after_ref[span], to_heads)
        gated = head * gate
        squares = jnp.sum(gated * gated, axis=1, keepdims=True)
        sq_send[c] = jnp.broadcast_to(squares, sq_send.shape[1:])
        if c == 0:
            pl.semaphore_wait(barrier, fars // 2 + groups)
        sq_copies[c].start()
        weighted_buf[span] = values * dot_split(keep_ref[span], to_heads)
        return (gated * gain_ref[...]).astype(BF16)

    sq_copies = [
        remote(sq_send.at[c], sq_recv.at[c], sq_sems, c, partner) for c in range(chunks)
    ]
    y_copies = [
        remote(zf_send.at[across_first[c]], zf_recv.at[across_first[c]], y_sems, c, device(mate))
        if c in across_first
        else remote(y_send.at[c], y_recv.at[c], y_sems, c, partner)
        for c in range(chunks)
    ]
    n_copies = [
        [
            remote(
                zn_send.at[across_first[c], step] if c in across_first else n_send.at[c, step],
                zn_recv.at[across_first[c], step] if c in across_first else n_recv.at[c, step],
                n_sems,
                c * (team - 1) + step,
                device(peer_at(step)),
            )
            for step in range(team - 1)
        ]
        for c in range(chunks)
    ]
    f_copies = [
        remote(
            f_send.at[c],
            f_recv.at[c],
            f_sems,
            c,
            partner if c in across_first else device(mate),
        )
        for c in range(chunks)
    ]

    def region(c, plane, owner):
        return out_buf.at[pl.ds(c * height, height), cols(plane * half + owner * width, width)]

    def owned(c, owner, sems, index, device, plane=near):
        return remote(region(c, plane, owner), region(c, plane, owner), sems, index, device)

    def send_partial(c):
        rows_in = front(c)
        if c in across_first:
            zacc_buf[across_first[c], 1] = dot(rows_in, weight_ref[:, cols((1 - near) * half, half)])
            zacc_buf[across_first[c], 0] = dot(rows_in, weight_ref[:, cols(near * half, half)])
            return
        y_send[c] = dot(rows_in, weight_ref[:, cols((1 - near) * half, half)]).astype(BF16)
        y_copies[c].start()
        acc_buf[c] = dot(rows_in, weight_ref[:, cols(near * half, half)])

    def row_scale(c):
        span = slice(c * height, (c + 1) * height)
        sq_copies[c].wait_recv()
        total = (sq_send[c] + sq_recv[c])[:, :1] / (2 * inner)
        return lax.rsqrt(total + EPSILON) * valid_ref[span, :1]

    def across_scale(c):
        k = across_first[c]
        scale = row_scale(c)
        for plane in range(2):
            zacc_buf[k, plane] = zacc_buf[k, plane] * scale
        for step in range(team - 1):
            place = peer_at(step)
            for plane in range(2):
                for slot, owner in enumerate((place, across(place))):
                    block = zacc_buf[k, plane, :, cols(owner * width, width)]
                    zn_send[k, step, plane, slot] = block.astype(BF16)
            n_copies[c][step].start()

    def across_team(c):
        k = across_first[c]
        for plane in range(2):
            own = zacc_buf[k, plane, :, cols(far * width, width)]
            other = zacc_buf[k, plane, :, cols(mate * width, width)]
            for step in range(team - 1):
                if plane == 0:
                    n_copies[c][step].wait_recv()
                own = own + zn_recv[k, step, plane, 0].astype(F32)
                other = other + zn_recv[k, step, plane, 1].astype(F32)
            zf_send[k, plane] = other.astype(BF16)
            zacc_buf[k, plane, :, cols(far * width, width)] = own
        y_copies[c].start()

    def across_pair(c):
        k = across_first[c]
        y_copies[c].wait_recv()
        own = zacc_buf[k, 0, :, cols(far * width, width)] + zf_recv[k, 0].astype(F32)
        other = zacc_buf[k, 1, :, cols(far * width, width)] + zf_recv[k, 1].astype(F32)
        f_send[c] = other.astype(BF16)
        f_copies[c].start()
        acc_buf[c, :, cols(far * width, width)] = own

    def pair_sum(c):
        scale = row_scale(c)
        y_copies[c].wait_recv()
        acc_buf[c] = (acc_buf[c] + y_recv[c].astype(F32)) * scale

        for step in range(team - 1):
            place = peer_at(step)
            n_send[c, step, 0] = acc_buf[c, :, cols(place * width, width)].astype(BF16)
            n_send[c, step, 1] = acc_buf[c, :, cols(across(place) * width, width)].astype(BF16)
            n_copies[c][step].start()

    def team_sum(c):
        own = acc_buf[c, :, cols(far * width, width)]
        other = acc_buf[c, :, cols(mate * width, width)]
        for step in range(team - 1):
            n_copies[c][step].wait_recv()
            own = own + n_recv[c, step, 0].astype(F32)
            other = other + n_recv[c, step, 1].astype(F32)
        f_send[c] = other.astype(BF16)
        f_copies[c].start()
        acc_buf[c, :, cols(far * width, width)] = own

    sent = []

    def send(copy):
        copy.start()
        sent.append(copy)

    per_o, per_p = 2 * team - 1, 2 * team

    def send_final(c):
        f_copies[c].wait_recv()
        total = acc_buf[c, :, cols(far * width, width)] + f_recv[c].astype(F32)
        span = pl.ds(c * height, height)
        out_buf[span, cols(near * half + far * width, width)] = total.astype(BF16)
        send(owned(c, far, o_sems, c * per_o, device(mate)))
        for step in range(team - 1):
            send(owned(c, far, o_sems, c * per_o + 1 + step, device(peer_at(step))))
        send(owned(c, far, p_sems, c * per_p, partner))

    def forward(c):
        owned(c, mate, o_sems, c * per_o, partner).wait_recv()
        for step in range(team - 1):
            send(owned(c, mate, o_sems, c * per_o + team + step, device(peer_at(step))))
        send(owned(c, mate, p_sems, c * per_p + 1, partner))
        for step in range(team - 1):
            place = peer_of(step)
            owned(c, place, o_sems, c * per_o + 1 + step, partner).wait_recv()
            send(owned(c, place, p_sems, c * per_p + 2 + step, partner))

    def forward_last(c):
        for step in range(team - 1):
            place = across(peer_of(step))
            owned(c, place, o_sems, c * per_o + team + step, partner).wait_recv()
            send(owned(c, place, p_sems, c * per_p + team + 1 + step, partner))

    def complete(c):
        places = [far, mate]
        places += [peer_of(step) for step in range(team - 1)]
        places += [across(peer_of(step)) for step in range(team - 1)]
        for index, place in enumerate(places):
            owned(c, place, p_sems, c * per_p + index, partner, 1 - near).wait_recv()

    def keep_state(c):
        for r in range(c * per_chunk, (c + 1) * per_chunk):
            span = slice(r * positions, (r + 1) * positions)
            added = dot_tn(weighted_buf[span].astype(BF16), input_map[span])
            for h in range(heads):
                block = slice(h * head_dim, (h + 1) * head_dim)
                kept_buf[r, block] = (
                    scale_ref[r, h] * state_buf[r, block].astype(F32) + added[block]
                ).astype(BF16)

    hop, wire = 2.7, 0.7 * height / 32
    events = []
    ready = 4 * wire
    for c in range(chunks):
        begin = 2.0 * c
        events.append((begin, c, send_partial))
        if c in across_first:
            kind = across_first[c]
            scaled = begin + 4.0
            teamed = scaled + 4 * wire * (1 + kind) + hop
            paired = teamed + 2 * wire + hop
            summed = paired + wire + hop
            events += [(scaled, c, across_scale), (teamed, c, across_team)]
            events.append((paired, c, across_pair))
        else:
            paired = max(begin + 4 * wire, ready) + hop
            ready = ready + 4 * wire
            teamed = paired + 2 * wire + hop
            summed = teamed + wire + hop
            events += [(paired, c, pair_sum), (teamed, c, team_sum)]
        events.append((summed, c, send_final))
        events.append((summed + wire + hop, c, forward))
        events.append((summed + 2 * (wire + hop), c, forward_last))
        events.append((16.0 + 1.4 * c, c, keep_state))
        events.append((100.0 + c, c, complete))
    events.sort(key=lambda event: event[:2])
    count_copies = []
    for _, c, stage in events:
        stage(c)
        if stage is send_partial and c == 0:
            for hop in range(groups - 1):
                copy = pltpu.make_async_remote_copy(
                    src_ref=count_ref,
                    dst_ref=count_recv.at[hop],
                    send_sem=count_sems.at[0, hop],
                    recv_sem=count_sems.at[1, hop],
                    device_id={"dp": lax.rem(group + 1 + hop, groups)},
                    device_id_type=MESH,
                )
                copy.start()
                count_copies.append(copy)

    count = count_ref[...]
    for hop in range(groups - 1):
        count_copies[hop].wait_recv()
        count = count + count_recv[hop]
    total_ref[0] = count[0, 0]

    for copy in sq_copies + y_copies + sum(n_copies, []) + f_copies + sent + count_copies:
        copy.wait_send()


def finish_kernel(
    rows_ref,
    kept_ref,
    inner_ref,
    cache_ref,
    group_proj_ref,
    group_cache_ref,
    fresh_pick_ref,
    cache_pick_ref,
    rows_hbm,
    kept_hbm,
    value_kept_hbm,
    group_kept_hbm,
    value_kept_ref,
    group_kept_ref,
    sems,
):
    copies = [
        pltpu.make_async_copy(rows_ref, rows_hbm, sems.at[0]),
        pltpu.make_async_copy(kept_ref, kept_hbm, sems.at[1]),
        pltpu.make_async_copy(value_kept_ref, value_kept_hbm, sems.at[2]),
        pltpu.make_async_copy(group_kept_ref, group_kept_hbm, sems.at[3]),
    ]
    copies[0].start()
    copies[1].start()
    def kept(fresh, cache, target, copy):
        flat = cache.reshape(-1, cache.shape[2])
        rows = dot(fresh_pick_ref[...], fresh) + dot(cache_pick_ref[...], flat)
        target[...] = rows.reshape(target.shape).astype(BF16)
        copy.start()

    kept(inner_ref[1], cache_ref[...], value_kept_ref, copies[2])
    kept(group_proj_ref[...], group_cache_ref[...], group_kept_ref, copies[3])
    for copy in copies:
        copy.wait()


def local(
    tokens,
    norm_gain,
    in_weight,
    group_weight,
    step_weight,
    value_kernel,
    value_offset,
    group_kernel,
    group_offset,
    step_bias,
    decay_rate,
    skip_gain,
    out_gain,
    out_weight,
    scan_state,
    value_cache,
    group_cache,
    accepted,
    draft_lengths,
    live_flags,
):
    requests, positions, model_width = tokens.shape
    rows = requests * positions
    heads, head_dim, state_size = scan_state.shape[1:]
    inner = heads * head_dim
    map_width = group_weight.shape[1]
    depth = value_cache.shape[1]
    lanes = positions * heads
    groups = lax.axis_size("dp")
    chunks = next(c for c in (6, 4, 3, 2, 1) if requests % c == 0 and (rows // c) % 16 == 0)
    height = rows // chunks
    half = model_width // 2
    vmem = pl.BlockSpec(memory_space=pltpu.VMEM)
    smem = pl.BlockSpec(memory_space=pltpu.SMEM)
    hbm = pl.BlockSpec(memory_space=pltpu.HBM)

    def pinned(array):
        return pltpu.with_memory_space_constraint(array, pltpu.HBM)

    def shaped(dims, kind):
        return jax.ShapeDtypeStruct(dims, kind)

    (
        normed,
        input_map,
        output_map,
        group_proj,
        mix,
        keep,
        after,
        kept_scale,
        valid,
        fresh_pick,
        cache_pick,
        own_total,
        in_weight,
        out_weight,
    ) = pl.pallas_call(
        prepare_kernel,
        out_shape=[
            shaped((rows, model_width), BF16),
            shaped((rows, map_width), BF16),
            shaped((rows, map_width), BF16),
            shaped((rows, map_width), BF16),
            shaped((rows, lanes), F32),
            shaped((rows, lanes), F32),
            shaped((rows, lanes), F32),
            shaped((requests, heads), F32),
            shaped((rows, 128), F32),
            shaped((depth * requests, rows), BF16),
            shaped((depth * requests, depth * requests), BF16),
            shaped((8, 128), jnp.int32),
            shaped(in_weight.shape, BF16),
            shaped(out_weight.shape, BF16),
        ],
        in_specs=[hbm] * 14,
        out_specs=[vmem] * 14,
        scratch_shapes=[
            pltpu.SMEM((requests,), jnp.int32),
            pltpu.SMEM((requests,), jnp.int32),
            pltpu.SMEM((requests,), jnp.int32),
            pltpu.VMEM((rows, model_width), BF16),
            pltpu.VMEM((1, model_width), F32),
            pltpu.VMEM(group_weight.shape, BF16),
            pltpu.VMEM(step_weight.shape[::-1], BF16),
            pltpu.VMEM((depth, requests, map_width), BF16),
            pltpu.VMEM(group_kernel.shape, BF16),
            pltpu.VMEM((1, map_width), BF16),
            pltpu.VMEM((1, heads), F32),
            pltpu.VMEM((1, heads), F32),
            pltpu.VMEM((rows, map_width), BF16),
            pltpu.VMEM((rows, map_width), BF16),
            pltpu.SemaphoreType.DMA((12,)),
            pltpu.SemaphoreType.DMA((2,)),
            pltpu.SemaphoreType.DMA((2,)),
        ],
        compiler_params=pltpu.CompilerParams(
            collective_id=1, has_side_effects=True, vmem_limit_bytes=20 * 1024 * 1024
        ),
    )(
        pinned(accepted),
        pinned(draft_lengths),
        pinned(live_flags),
        pinned(tokens.reshape(rows, model_width)),
        pinned(norm_gain.reshape(1, -1)),
        pinned(group_weight),
        pinned(step_weight.T),
        pinned(jnp.transpose(group_cache, (1, 0, 2))),
        pinned(group_kernel),
        pinned(group_offset.reshape(1, -1)),
        pinned(step_bias.reshape(1, -1)),
        pinned(decay_rate.reshape(1, -1)),
        pinned(in_weight),
        pinned(out_weight),
    )
    normed, value_offset = lax.optimization_barrier((normed, value_offset))
    inner_proj = jnp.einsum(
        "rd,dgi->gri", normed, in_weight, preferred_element_type=F32
    ).astype(BF16)

    cache_rows = jnp.transpose(value_cache, (1, 0, 2))
    fars = lax.axis_size("tensor") // 2
    team = fars // 2
    width = half // fars
    kinds = max(1, len(across_first_chunks(chunks)))
    out_rows, kept_state, totals = pl.pallas_call(
        layer_kernel,
        out_shape=[
            shaped((rows, model_width), BF16),
            shaped((requests, inner, state_size), BF16),
            shaped((1,), jnp.int32),
        ],
        in_specs=[smem] * 2 + [vmem] * 13 + [hbm],
        out_specs=[vmem, vmem, smem],
        scratch_shapes=[
            pltpu.VMEM((requests, inner, state_size), BF16),
            pltpu.VMEM((chunks, height, half), BF16),
            pltpu.VMEM((chunks, height, half), BF16),
            pltpu.VMEM((chunks, team - 1, 2, height, width), BF16),
            pltpu.VMEM((chunks, team - 1, 2, height, width), BF16),
            pltpu.VMEM((chunks, height, width), BF16),
            pltpu.VMEM((chunks, height, width), BF16),
            pltpu.VMEM((chunks, height, half), F32),
            pltpu.VMEM((kinds, team - 1, 2, 2, height, width), BF16),
            pltpu.VMEM((kinds, team - 1, 2, 2, height, width), BF16),
            pltpu.VMEM((kinds, 2, height, width), BF16),
            pltpu.VMEM((kinds, 2, height, width), BF16),
            pltpu.VMEM((kinds, 2, height, half), F32),
            pltpu.VMEM((positions, lanes, inner), BF16),
            pltpu.VMEM((rows, inner), F32),
            pltpu.VMEM((chunks, height, 128), F32),
            pltpu.VMEM((chunks, height, 128), F32),
            pltpu.VMEM((groups - 1, 8, 128), jnp.int32),
            pltpu.SemaphoreType.DMA((chunks,)),
            pltpu.SemaphoreType.DMA((2, chunks)),
            pltpu.SemaphoreType.DMA((2, chunks)),
            pltpu.SemaphoreType.DMA((2, chunks * (team - 1))),
            pltpu.SemaphoreType.DMA((2, chunks)),
            pltpu.SemaphoreType.DMA((2, chunks * (2 * team - 1))),
            pltpu.SemaphoreType.DMA((2, chunks * 2 * team)),
            pltpu.SemaphoreType.DMA((2, groups - 1)),
        ],
        compiler_params=pltpu.CompilerParams(
            collective_id=0, has_side_effects=True, vmem_limit_bytes=32 * 1024 * 1024
        ),
    )(
        kept_scale,
        skip_gain,
        inner_proj,
        input_map,
        output_map,
        mix,
        keep,
        after,
        valid,
        cache_rows,
        value_kernel,
        value_offset.reshape(1, -1),
        out_gain.reshape(1, -1),
        own_total,
        out_weight,
        pinned(scan_state.reshape(requests, inner, state_size)),
    )
    group_rows = jnp.transpose(group_cache, (1, 0, 2))
    out_rows, kept_state, value_kept, group_kept = pl.pallas_call(
        finish_kernel,
        out_shape=[
            pltpu.HBM((rows, model_width), BF16),
            pltpu.HBM((requests, inner, state_size), BF16),
            pltpu.HBM((depth, requests, inner), BF16),
            pltpu.HBM((depth, requests, map_width), BF16),
        ],
        in_specs=[vmem] * 8,
        out_specs=[hbm] * 4,
        scratch_shapes=[
            pltpu.VMEM((depth, requests, inner), BF16),
            pltpu.VMEM((depth, requests, map_width), BF16),
            pltpu.SemaphoreType.DMA((4,)),
        ],
        compiler_params=pltpu.CompilerParams(vmem_limit_bytes=16 * 1024 * 1024),
    )(
        out_rows,
        kept_state,
        inner_proj,
        cache_rows,
        group_proj,
        group_rows,
        fresh_pick,
        cache_pick,
    )
    return (
        out_rows.reshape(requests, positions, model_width),
        kept_state.reshape(scan_state.shape),
        jnp.transpose(value_kept, (1, 0, 2)),
        jnp.transpose(group_kept, (1, 0, 2)),
        totals,
    )


def solution(mesh):
    placed = (
        P("dp", None, None),
        P(),
        P(None, None, "tensor"),
        P(None, "tensor"),
        P(None, "tensor"),
        P(None, "tensor"),
        P("tensor"),
        P(None, "tensor"),
        P("tensor"),
        P("tensor"),
        P("tensor"),
        P("tensor"),
        P("tensor"),
        P("tensor", None),
        P("dp", "tensor", None, None),
        P("dp", None, "tensor"),
        P("dp", None, "tensor"),
        P("dp"),
        P("dp"),
        P("dp"),
    )
    return jax.shard_map(
        local,
        mesh=mesh,
        in_specs=placed,
        out_specs=(
            P("dp", None, None),
            P("dp", "tensor", None, None),
            P("dp", None, "tensor"),
            P("dp", None, "tensor"),
            P(),
        ),
        check_vma=False,
    )
```

```python
import jax
import jax.numpy as jnp
from jax import lax
from jax.experimental import pallas as pl
from jax.experimental.pallas import tpu as pltpu
from jax.sharding import PartitionSpec as P

EPSILON = 1e-05
MESH = pl.DeviceIdType.MESH
F32 = jnp.float32
BF16 = jnp.bfloat16


def iota(shape, axis):
    return lax.broadcasted_iota(jnp.int32, shape, axis)


def dot(a, b):
    return jnp.dot(a, b, preferred_element_type=F32)


def dot_nt(a, b):
    return lax.dot_general(a, b, (((1,), (1,)), ((), ())), preferred_element_type=F32)


def dot_tn(a, b):
    return lax.dot_general(a, b, (((0,), (0,)), ((), ())), preferred_element_type=F32)


def dot_split(a, b):
    high = a.astype(BF16)
    low = (a - high.astype(F32)).astype(BF16)
    return dot(high, b) + dot(low, b)


def silu(v):
    return v * (1.0 / (1.0 + jnp.exp(-v)))


def spread_cache(cache, rows, positions, first):
    depth, requests, width = cache.shape
    flat = cache.reshape(depth * requests, width)
    row = iota((rows, depth * requests), 0)
    col = iota((rows, depth * requests), 1)
    place = row % positions - (positions - depth)
    chosen = (col == place * requests + first + row // positions) & (place >= 0)
    return dot(chosen.astype(BF16), flat)


def convolve(fresh, cached, kernel, offset, positions):
    rows, width = fresh.shape
    taps = kernel.shape[0]
    fresh = fresh.reshape(rows // positions, positions, width)
    cached = cached.reshape(rows // positions, positions, width)
    place = iota(fresh.shape, 1)
    total = offset[None] + kernel[taps - 1 : taps][None] * fresh
    for shift in range(1, taps):
        merged = jnp.where(place < positions - shift, fresh, cached)
        moved = pltpu.roll(merged, shift, axis=1)
        total = total + kernel[taps - 1 - shift : taps - shift][None] * moved
    return silu(total).reshape(rows, width)


def prepare_kernel(
    accepted_hbm,
    draft_hbm,
    live_hbm,
    tokens_hbm,
    gain_hbm,
    weight_hbm,
    step_weight_hbm,
    cache_hbm,
    kernel_hbm,
    offset_hbm,
    bias_hbm,
    rate_hbm,
    in_weight_hbm,
    normed_ref,
    input_map_ref,
    output_map_ref,
    group_proj_ref,
    mix_ref,
    keep_ref,
    after_ref,
    scale_ref,
    valid_ref,
    fresh_pick_ref,
    cache_pick_ref,
    total_ref,
    in_weight_ref,
    accepted_ref,
    draft_ref,
    live_ref,
    tokens_ref,
    gain_ref,
    weight_ref,
    step_weight_ref,
    cache_ref,
    kernel_ref,
    offset_ref,
    bias_ref,
    rate_ref,
    map_send,
    map_recv,
    load_sems,
    map_sems,
    weight_sem,
):
    me = lax.axis_index("tensor")
    near = me % 2
    partner = me + 1 - 2 * near
    barrier = pltpu.get_barrier_semaphore()
    pl.semaphore_signal(barrier, inc=1, device_id={"tensor": partner}, device_id_type=MESH)
    sources = (gain_hbm, tokens_hbm, weight_hbm, step_weight_hbm, cache_hbm)
    sources += (kernel_hbm, offset_hbm, bias_hbm, rate_hbm, accepted_hbm, draft_hbm, live_hbm)
    targets = (gain_ref, tokens_ref, weight_ref, step_weight_ref, cache_ref)
    targets += (kernel_ref, offset_ref, bias_ref, rate_ref, accepted_ref, draft_ref, live_ref)
    loads = [
        pltpu.make_async_copy(source, target, load_sems.at[index])
        for index, (source, target) in enumerate(zip(sources, targets))
    ]
    for load in loads:
        load.start()
    rows, model_width = tokens_ref.shape
    requests = accepted_ref.shape[0]
    positions = rows // requests
    heads = bias_ref.shape[1]
    depth = cache_ref.shape[0]
    lanes = positions * heads
    step = 16 if rows % 16 == 0 else 8
    loads[0].wait()
    loads[1].wait()
    weight_loads = [
        pltpu.make_async_copy(in_weight_hbm, in_weight_ref, weight_sem.at[0]),
    ]
    for load in weight_loads:
        load.start()
    for start in range(0, rows, step):
        wide = tokens_ref[start : start + step].astype(F32)
        mean = jnp.sum(wide * wide, axis=1, keepdims=True) / model_width
        normed_ref[start : start + step] = (
            wide * lax.rsqrt(mean + EPSILON) * gain_ref[...]
        ).astype(BF16)
    for load in loads[2:]:
        load.wait()
    normed = normed_ref[...]
    group_proj = dot(normed, weight_ref[...]).astype(BF16)
    group_proj_ref[...] = group_proj

    cache = cache_ref[...]
    cached = spread_cache(cache, rows, positions, 0)
    conv = convolve(
        group_proj.astype(F32),
        cached,
        kernel_ref[...].astype(F32),
        offset_ref[...].astype(F32),
        positions,
    )
    map_send[...] = conv.astype(BF16)
    pl.semaphore_wait(barrier, 1)
    map_copy = pltpu.make_async_remote_copy(
        src_ref=map_send,
        dst_ref=map_recv,
        send_sem=map_sems.at[0],
        recv_sem=map_sems.at[1],
        device_id={"tensor": partner},
        device_id_type=MESH,
    )
    map_copy.start()
    step_raw = dot_nt(normed, step_weight_ref[...])

    counts = [accepted_ref[r] * live_ref[r] for r in range(requests)]
    total = counts[0]
    for count in counts[1:]:
        total = total + count
    total_ref[...] = jnp.full(total_ref.shape, total, jnp.int32)

    bias = jnp.concatenate([bias_ref[...]] * positions, axis=1)[None]
    rate = jnp.concatenate([rate_ref[...]] * positions, axis=1)[None]
    raw = jnp.concatenate([step_raw] * positions, axis=1).reshape(requests, positions, lanes)
    raw = raw + bias
    size = jnp.maximum(raw, 0.0) + jnp.log1p(jnp.exp(-jnp.abs(raw)))
    log_decay = -size * rate
    place = iota((requests, positions, lanes), 1)
    source = iota((requests, positions, lanes), 2) // heads
    after = log_decay
    shift = 1
    while shift < positions:
        after = after + jnp.where(place >= shift, pltpu.roll(after, shift, axis=1), 0.0)
        shift *= 2
    kept = jnp.stack([jnp.full((positions, lanes), count, jnp.int32) for count in counts])
    own = place == source
    after_source = jnp.sum(jnp.where(own, after, 0.0), axis=1, keepdims=True)
    size_source = jnp.sum(jnp.where(own, size, 0.0), axis=1, keepdims=True)
    causal = place >= source
    mix = jnp.where(causal, jnp.exp(jnp.where(causal, after - after_source, 0.0)), 0.0) * size_source
    kept_after = jnp.sum(jnp.where(place == kept - 1, after, 0.0), axis=1, keepdims=True)
    before = place < kept
    keep = jnp.where(before, jnp.exp(jnp.where(before, kept_after - after, 0.0)), 0.0) * size
    mix_ref[...] = mix.reshape(rows, lanes)
    keep_ref[...] = keep.reshape(rows, lanes)
    after_ref[...] = jnp.exp(after).reshape(rows, lanes)
    scale_ref[...] = jnp.exp(kept_after[:, 0, :heads])

    wide_lanes = valid_ref.shape[1]
    drafted = jnp.stack(
        [
            jnp.full((positions, wide_lanes), draft_ref[r] * (live_ref[r] == 1).astype(jnp.int32), jnp.int32)
            for r in range(requests)
        ]
    )
    valid = iota(drafted.shape, 1) < drafted
    valid_ref[...] = valid.astype(F32).reshape(rows, wide_lanes)

    def picks(width, position_of, request_of):
        shape = (requests, width)
        row = iota(shape, 0)
        count = jnp.zeros(shape, jnp.int32)
        for r in range(requests):
            count = jnp.where(row == r, counts[r], count)
        col = iota(shape, 1)
        return jnp.concatenate(
            [
                ((position_of(col) == count + t) & (request_of(col) == row)).astype(F32)
                for t in range(depth)
            ],
            axis=0,
        ).astype(BF16)

    fresh_pick = picks(rows, lambda col: col % positions + depth, lambda col: col // positions)
    cache_pick = picks(depth * requests, lambda col: col // requests, lambda col: col % requests)
    fresh_pick_ref[...] = fresh_pick
    cache_pick_ref[...] = cache_pick
    map_copy.wait_recv()
    mine, other = map_send[...].astype(F32), map_recv[...].astype(F32)
    input_map_ref[...] = jnp.where(near == 0, mine, other).astype(BF16)
    output_map_ref[...] = jnp.where(near == 0, other, mine).astype(BF16)
    map_copy.wait_send()
    for load in weight_loads:
        load.wait()


def across_first_chunks(chunks):
    return {1: 0} if chunks >= 6 else {}


def layer_kernel(
    scale_ref,
    skip_ref,
    inner_ref,
    input_map,
    output_map,
    mix_ref,
    keep_ref,
    after_ref,
    valid_ref,
    cache_ref,
    kernel_ref,
    offset_ref,
    gain_ref,
    count_ref,
    weight_ref,
    state_hbm,
    out_buf,
    kept_buf,
    total_ref,
    state_buf,
    y_send,
    y_recv,
    n_send,
    n_recv,
    f_send,
    f_recv,
    acc_buf,
    zn_send,
    zn_recv,
    zf_send,
    zf_recv,
    zacc_buf,
    place_buf,
    weighted_buf,
    sq_send,
    sq_recv,
    count_recv,
    state_sem,
    sq_sems,
    y_sems,
    n_sems,
    f_sems,
    o_sems,
    p_sems,
    count_sems,
):
    chunks, height, half = y_send.shape
    rows, inner = inner_ref.shape[1:]
    requests = state_buf.shape[0]
    positions = rows // requests
    lanes = mix_ref.shape[1]
    heads = lanes // positions
    head_dim = inner // heads
    per_chunk = requests // chunks
    across_first = across_first_chunks(chunks)
    direct = set(range(chunks - 2, chunks))
    depth = cache_ref.shape[0]

    members = lax.axis_size("tensor")
    fars = members // 2
    width = half // fars
    me = lax.axis_index("tensor")
    far, near = me // 2, me % 2
    partner = far * 2 + (1 - near)

    team = fars // 2
    wing, seat = far // team, far % team
    mate = (1 - wing) * team + seat

    def peer_at(step):
        return wing * team + lax.rem(seat + 1 + step, team)

    def peer_of(step):
        return wing * team + lax.rem(seat - 1 - step + 2 * team, team)

    def across(place):
        return lax.rem(place + team, fars)

    def device(place):
        return place * 2 + near

    groups = lax.axis_size("dp")
    group = lax.axis_index("dp")

    def cols(start, width):
        return pl.ds(pl.multiple_of(start, width), width)

    state_loads = [
        pltpu.make_async_copy(
            state_hbm.at[pl.ds(c * per_chunk, per_chunk)],
            state_buf.at[pl.ds(c * per_chunk, per_chunk)],
            state_sem.at[c],
        )
        for c in range(chunks)
    ]
    state_loads[0].start()
    for load in state_loads[1:]:
        load.start()

    barrier = pltpu.get_barrier_semaphore()
    pl.semaphore_signal(barrier, inc=1, device_id={"tensor": partner}, device_id_type=MESH)

    others = [mate] + [peer_at(step) for step in range(team - 1)]
    others += [across(peer_at(step)) for step in range(team - 1)]
    for place in others:
        pl.semaphore_signal(
            barrier, inc=1, device_id={"tensor": device(place)}, device_id_type=MESH
        )
    for hop in range(groups - 1):
        pl.semaphore_signal(
            barrier,
            inc=1,
            device_id={"dp": lax.rem(group + 1 + hop, groups)},
            device_id_type=MESH,
        )
    def remote(source, target, sems, index, device):
        return pltpu.make_async_remote_copy(
            src_ref=source,
            dst_ref=target,
            send_sem=sems.at[0, index],
            recv_sem=sems.at[1, index],
            device_id={"tensor": device},
            device_id_type=MESH,
        )

    shape = (lanes, inner)
    target_head = iota(shape, 1) // head_dim
    lane_row = iota(shape, 0)
    for j in range(positions):
        place_buf[j] = (lane_row == target_head + j * heads).astype(F32).astype(BF16)
    to_heads = place_buf[0]

    lane_head = iota((1, inner), 1) // head_dim
    skip = jnp.zeros((1, inner), F32)
    for h in range(heads):
        skip = jnp.where(lane_head == h, skip_ref[h], skip)

    cache = cache_ref[...]
    kernel = kernel_ref[...].astype(F32)
    offset = offset_ref[...].astype(F32)

    def values_of(c):
        span = slice(c * height, (c + 1) * height)
        cached = spread_cache(cache, height, positions, c * per_chunk)
        return convolve(inner_ref[1, span].astype(F32), cached, kernel, offset, positions)

    def front(c):
        span = slice(c * height, (c + 1) * height)
        values = values_of(c)
        gate = silu(inner_ref[0, span].astype(F32))
        align = dot_nt(output_map[span], input_map[span])
        square = (height, height)
        same = iota(square, 0) // positions == iota(square, 1) // positions
        fold = (height, lanes)
        folded = (iota(fold, 0) % positions == iota(fold, 1) // heads).astype(F32).astype(BF16)
        mix = (mix_ref[span] * dot_split(jnp.where(same, align, 0.0), folded)).astype(BF16)
        values3 = values.reshape(per_chunk, positions, inner)
        head = skip * values
        for j in range(positions):
            spread = jnp.broadcast_to(values3[:, j : j + 1], values3.shape).reshape(height, inner)
            head = head + dot(mix, place_buf[j]) * spread
        state_loads[c].wait()
        outputs = output_map[span].astype(F32)
        carried = jnp.concatenate(
            [
                dot_nt(
                    outputs[(r - c * per_chunk) * positions :][:positions].astype(BF16), state_buf[r]
                )
                for r in range(c * per_chunk, (c + 1) * per_chunk)
            ],
            axis=0,
        )
        head = head + carried * dot_split(after_ref[span], to_heads)
        gated = head * gate
        squares = jnp.sum(gated * gated, axis=1, keepdims=True)
        sq_send[c] = jnp.broadcast_to(squares, sq_send.shape[1:])
        if c == 0:
            pl.semaphore_wait(barrier, fars + groups - 1)
        sq_copies[c].start()
        weighted_buf[span] = values * dot_split(keep_ref[span], to_heads)
        return (gated * gain_ref[...]).astype(BF16)

    sq_copies = [
        remote(sq_send.at[c], sq_recv.at[c], sq_sems, c, partner) for c in range(chunks)
    ]
    y_copies = [
        remote(zf_send.at[across_first[c]], zf_recv.at[across_first[c]], y_sems, c, device(mate))
        if c in across_first
        else remote(y_send.at[c], y_recv.at[c], y_sems, c, partner)
        for c in range(chunks)
    ]
    n_copies = [
        [
            remote(
                zn_send.at[across_first[c], step] if c in across_first else n_send.at[c, step],
                zn_recv.at[across_first[c], step] if c in across_first else n_recv.at[c, step],
                n_sems,
                c * (team - 1) + step,
                device(peer_at(step)),
            )
            for step in range(team - 1)
        ]
        for c in range(chunks)
    ]
    f_copies = [
        remote(
            f_send.at[c],
            f_recv.at[c],
            f_sems,
            c,
            partner if c in across_first else device(mate),
        )
        for c in range(chunks)
    ]

    def region(c, plane, owner):
        return out_buf.at[pl.ds(c * height, height), cols(plane * half + owner * width, width)]

    def owned(c, owner, sems, index, device, plane=near):
        return remote(region(c, plane, owner), region(c, plane, owner), sems, index, device)

    def send_partial(c):
        rows_in = front(c)
        if c in across_first:
            zacc_buf[across_first[c], 1] = dot(rows_in, weight_ref[:, cols((1 - near) * half, half)])
            zacc_buf[across_first[c], 0] = dot(rows_in, weight_ref[:, cols(near * half, half)])
            return
        y_send[c] = dot(rows_in, weight_ref[:, cols((1 - near) * half, half)]).astype(BF16)
        y_copies[c].start()
        acc_buf[c] = dot(rows_in, weight_ref[:, cols(near * half, half)])

    def row_scale(c):
        span = slice(c * height, (c + 1) * height)
        sq_copies[c].wait_recv()
        total = (sq_send[c] + sq_recv[c])[:, :1] / (2 * inner)
        return lax.rsqrt(total + EPSILON) * valid_ref[span, :1]

    def across_scale(c):
        k = across_first[c]
        scale = row_scale(c)
        for plane in range(2):
            zacc_buf[k, plane] = zacc_buf[k, plane] * scale
        for step in range(team - 1):
            place = peer_at(step)
            for plane in range(2):
                for slot, owner in enumerate((place, across(place))):
                    block = zacc_buf[k, plane, :, cols(owner * width, width)]
                    zn_send[k, step, plane, slot] = block.astype(BF16)
            n_copies[c][step].start()

    def across_team(c):
        k = across_first[c]
        for plane in range(2):
            own = zacc_buf[k, plane, :, cols(far * width, width)]
            other = zacc_buf[k, plane, :, cols(mate * width, width)]
            for step in range(team - 1):
                if plane == 0:
                    n_copies[c][step].wait_recv()
                own = own + zn_recv[k, step, plane, 0].astype(F32)
                other = other + zn_recv[k, step, plane, 1].astype(F32)
            zf_send[k, plane] = other.astype(BF16)
            zacc_buf[k, plane, :, cols(far * width, width)] = own
        y_copies[c].start()

    def across_pair(c):
        k = across_first[c]
        y_copies[c].wait_recv()
        own = zacc_buf[k, 0, :, cols(far * width, width)] + zf_recv[k, 0].astype(F32)
        other = zacc_buf[k, 1, :, cols(far * width, width)] + zf_recv[k, 1].astype(F32)
        f_send[c] = other.astype(BF16)
        f_copies[c].start()
        acc_buf[c, :, cols(far * width, width)] = own

    def pair_sum(c):
        scale = row_scale(c)
        y_copies[c].wait_recv()
        acc_buf[c] = (acc_buf[c] + y_recv[c].astype(F32)) * scale

        for step in range(team - 1):
            place = peer_at(step)
            n_send[c, step, 0] = acc_buf[c, :, cols(place * width, width)].astype(BF16)
            n_send[c, step, 1] = acc_buf[c, :, cols(across(place) * width, width)].astype(BF16)
            n_copies[c][step].start()

    def team_sum(c):
        own = acc_buf[c, :, cols(far * width, width)]
        other = acc_buf[c, :, cols(mate * width, width)]
        for step in range(team - 1):
            n_copies[c][step].wait_recv()
            own = own + n_recv[c, step, 0].astype(F32)
            other = other + n_recv[c, step, 1].astype(F32)
        f_send[c] = other.astype(BF16)
        f_copies[c].start()
        acc_buf[c, :, cols(far * width, width)] = own

    sent = []

    def send(copy):
        copy.start()
        sent.append(copy)

    per_o, per_p = 2 * team - 1, 2 * team

    def send_final(c):
        f_copies[c].wait_recv()
        total = acc_buf[c, :, cols(far * width, width)] + f_recv[c].astype(F32)
        span = pl.ds(c * height, height)
        out_buf[span, cols(near * half + far * width, width)] = total.astype(BF16)
        send(owned(c, far, o_sems, c * per_o, device(mate)))
        for step in range(team - 1):
            send(owned(c, far, o_sems, c * per_o + 1 + step, device(peer_at(step))))
        if c in direct:
            for step in range(team - 1):
                target = device(across(peer_at(step)))
                send(owned(c, far, o_sems, c * per_o + team + step, target))
        send(owned(c, far, p_sems, c * per_p, partner))

    def forward(c):
        owned(c, mate, o_sems, c * per_o, partner).wait_recv()
        for step in range(team - 1 if c not in direct else 0):
            send(owned(c, mate, o_sems, c * per_o + team + step, device(peer_at(step))))
        send(owned(c, mate, p_sems, c * per_p + 1, partner))
        for step in range(team - 1):
            place = peer_of(step)
            owned(c, place, o_sems, c * per_o + 1 + step, partner).wait_recv()
            send(owned(c, place, p_sems, c * per_p + 2 + step, partner))

    def forward_last(c):
        for step in range(team - 1):
            place = across(peer_of(step))
            owned(c, place, o_sems, c * per_o + team + step, partner).wait_recv()
            send(owned(c, place, p_sems, c * per_p + team + 1 + step, partner))

    def complete(c):
        places = [far, mate]
        places += [peer_of(step) for step in range(team - 1)]
        places += [across(peer_of(step)) for step in range(team - 1)]
        for index, place in enumerate(places):
            owned(c, place, p_sems, c * per_p + index, partner, 1 - near).wait_recv()

    def keep_state(c):
        for r in range(c * per_chunk, (c + 1) * per_chunk):
            span = slice(r * positions, (r + 1) * positions)
            added = dot_tn(weighted_buf[span].astype(BF16), input_map[span])
            for h in range(heads):
                block = slice(h * head_dim, (h + 1) * head_dim)
                kept_buf[r, block] = (
                    scale_ref[r, h] * state_buf[r, block].astype(F32) + added[block]
                ).astype(BF16)

    hop, wire = 2.2, 0.7 * height / 32
    events = []
    ready = 4 * wire
    for c in range(chunks):
        begin = 2.0 * c
        events.append((begin, c, send_partial))
        if c in across_first:
            kind = across_first[c]
            scaled = begin + 4.0
            teamed = scaled + 4 * wire * (1 + kind) + hop
            paired = teamed + 2 * wire + hop
            summed = paired + wire + hop
            events += [(scaled, c, across_scale), (teamed, c, across_team)]
            events.append((paired, c, across_pair))
        else:
            paired = max(begin + 4 * wire, ready) + hop
            ready = ready + 4 * wire
            teamed = paired + 2 * wire + hop
            summed = teamed + wire + hop
            events += [(paired, c, pair_sum), (teamed, c, team_sum)]
        events.append((summed, c, send_final))
        events.append((summed + wire + hop, c, forward))
        last = summed + 3 * wire + hop + 0.8 if c in direct else summed + 2 * (wire + hop)
        events.append((last, c, forward_last))
        events.append((16.0 + 1.4 * c, c, keep_state))
        events.append((100.0 + c, c, complete))
    events.sort(key=lambda event: event[:2])
    count_copies = []
    for _, c, stage in events:
        stage(c)
        if stage is send_partial and c == 0:
            for hop in range(groups - 1):
                copy = pltpu.make_async_remote_copy(
                    src_ref=count_ref,
                    dst_ref=count_recv.at[hop],
                    send_sem=count_sems.at[0, hop],
                    recv_sem=count_sems.at[1, hop],
                    device_id={"dp": lax.rem(group + 1 + hop, groups)},
                    device_id_type=MESH,
                )
                copy.start()
                count_copies.append(copy)

    count = count_ref[...]
    for hop in range(groups - 1):
        count_copies[hop].wait_recv()
        count = count + count_recv[hop]
    total_ref[0] = count[0, 0]

    for copy in sq_copies + y_copies + sum(n_copies, []) + f_copies + sent + count_copies:
        copy.wait_send()


def finish_kernel(
    rows_ref,
    kept_ref,
    inner_ref,
    cache_ref,
    group_proj_ref,
    group_cache_ref,
    fresh_pick_ref,
    cache_pick_ref,
    rows_hbm,
    kept_hbm,
    value_kept_hbm,
    group_kept_hbm,
    value_kept_ref,
    group_kept_ref,
    sems,
):
    copies = [
        pltpu.make_async_copy(value_kept_ref, value_kept_hbm, sems.at[0]),
        pltpu.make_async_copy(group_kept_ref, group_kept_hbm, sems.at[1]),
    ]
    cuts = 4 if kept_ref.shape[0] % 4 == 0 and rows_ref.shape[0] % 64 == 0 else 1
    for source, target, base in ((kept_ref, kept_hbm, 2), (rows_ref, rows_hbm, 2 + cuts)):
        size = source.shape[0] // cuts
        for cut in range(cuts):
            span = pl.ds(cut * size, size)
            copy = pltpu.make_async_copy(source.at[span], target.at[span], sems.at[base + cut])
            copy.start()
            copies.append(copy)
    def kept(fresh, cache, target, copy):
        flat = cache.reshape(-1, cache.shape[2])
        rows = dot(fresh_pick_ref[...], fresh) + dot(cache_pick_ref[...], flat)
        target[...] = rows.reshape(target.shape).astype(BF16)
        copy.start()

    kept(inner_ref[1], cache_ref[...], value_kept_ref, copies[0])
    kept(group_proj_ref[...], group_cache_ref[...], group_kept_ref, copies[1])
    for copy in copies:
        copy.wait()


def local(
    tokens,
    norm_gain,
    in_weight,
    group_weight,
    step_weight,
    value_kernel,
    value_offset,
    group_kernel,
    group_offset,
    step_bias,
    decay_rate,
    skip_gain,
    out_gain,
    out_weight,
    scan_state,
    value_cache,
    group_cache,
    accepted,
    draft_lengths,
    live_flags,
):
    requests, positions, model_width = tokens.shape
    rows = requests * positions
    heads, head_dim, state_size = scan_state.shape[1:]
    inner = heads * head_dim
    map_width = group_weight.shape[1]
    depth = value_cache.shape[1]
    lanes = positions * heads
    groups = lax.axis_size("dp")
    chunks = next(c for c in (6, 4, 3, 2, 1) if requests % c == 0 and (rows // c) % 16 == 0)
    height = rows // chunks
    half = model_width // 2
    vmem = pl.BlockSpec(memory_space=pltpu.VMEM)
    smem = pl.BlockSpec(memory_space=pltpu.SMEM)
    hbm = pl.BlockSpec(memory_space=pltpu.HBM)

    def pinned(array):
        return pltpu.with_memory_space_constraint(array, pltpu.HBM)

    def shaped(dims, kind):
        return jax.ShapeDtypeStruct(dims, kind)

    (
        normed,
        input_map,
        output_map,
        group_proj,
        mix,
        keep,
        after,
        kept_scale,
        valid,
        fresh_pick,
        cache_pick,
        own_total,
        in_weight,
    ) = pl.pallas_call(
        prepare_kernel,
        out_shape=[
            shaped((rows, model_width), BF16),
            shaped((rows, map_width), BF16),
            shaped((rows, map_width), BF16),
            shaped((rows, map_width), BF16),
            shaped((rows, lanes), F32),
            shaped((rows, lanes), F32),
            shaped((rows, lanes), F32),
            shaped((requests, heads), F32),
            shaped((rows, 128), F32),
            shaped((depth * requests, rows), BF16),
            shaped((depth * requests, depth * requests), BF16),
            shaped((8, 128), jnp.int32),
            shaped(in_weight.shape, BF16),
        ],
        in_specs=[hbm] * 13,
        out_specs=[vmem] * 13,
        scratch_shapes=[
            pltpu.SMEM((requests,), jnp.int32),
            pltpu.SMEM((requests,), jnp.int32),
            pltpu.SMEM((requests,), jnp.int32),
            pltpu.VMEM((rows, model_width), BF16),
            pltpu.VMEM((1, model_width), F32),
            pltpu.VMEM(group_weight.shape, BF16),
            pltpu.VMEM(step_weight.shape[::-1], BF16),
            pltpu.VMEM((depth, requests, map_width), BF16),
            pltpu.VMEM(group_kernel.shape, BF16),
            pltpu.VMEM((1, map_width), BF16),
            pltpu.VMEM((1, heads), F32),
            pltpu.VMEM((1, heads), F32),
            pltpu.VMEM((rows, map_width), BF16),
            pltpu.VMEM((rows, map_width), BF16),
            pltpu.SemaphoreType.DMA((12,)),
            pltpu.SemaphoreType.DMA((2,)),
            pltpu.SemaphoreType.DMA((2,)),
        ],
        compiler_params=pltpu.CompilerParams(
            collective_id=1, has_side_effects=True, vmem_limit_bytes=20 * 1024 * 1024
        ),
    )(
        pinned(accepted),
        pinned(draft_lengths),
        pinned(live_flags),
        pinned(tokens.reshape(rows, model_width)),
        pinned(norm_gain.reshape(1, -1)),
        pinned(group_weight),
        pinned(step_weight.T),
        pinned(jnp.transpose(group_cache, (1, 0, 2))),
        pinned(group_kernel),
        pinned(group_offset.reshape(1, -1)),
        pinned(step_bias.reshape(1, -1)),
        pinned(decay_rate.reshape(1, -1)),
        pinned(in_weight),
    )
    normed, value_offset = lax.optimization_barrier((normed, value_offset))
    inner_proj = jnp.einsum(
        "rd,dgi->gri", normed, in_weight, preferred_element_type=F32
    ).astype(BF16)

    cache_rows = jnp.transpose(value_cache, (1, 0, 2))
    fars = lax.axis_size("tensor") // 2
    team = fars // 2
    width = half // fars
    kinds = max(1, len(across_first_chunks(chunks)))
    out_rows, kept_state, totals = pl.pallas_call(
        layer_kernel,
        out_shape=[
            shaped((rows, model_width), BF16),
            shaped((requests, inner, state_size), BF16),
            shaped((1,), jnp.int32),
        ],
        in_specs=[smem] * 2 + [vmem] * 13 + [hbm],
        out_specs=[vmem, vmem, smem],
        scratch_shapes=[
            pltpu.VMEM((requests, inner, state_size), BF16),
            pltpu.VMEM((chunks, height, half), BF16),
            pltpu.VMEM((chunks, height, half), BF16),
            pltpu.VMEM((chunks, team - 1, 2, height, width), BF16),
            pltpu.VMEM((chunks, team - 1, 2, height, width), BF16),
            pltpu.VMEM((chunks, height, width), BF16),
            pltpu.VMEM((chunks, height, width), BF16),
            pltpu.VMEM((chunks, height, half), F32),
            pltpu.VMEM((kinds, team - 1, 2, 2, height, width), BF16),
            pltpu.VMEM((kinds, team - 1, 2, 2, height, width), BF16),
            pltpu.VMEM((kinds, 2, height, width), BF16),
            pltpu.VMEM((kinds, 2, height, width), BF16),
            pltpu.VMEM((kinds, 2, height, half), F32),
            pltpu.VMEM((positions, lanes, inner), BF16),
            pltpu.VMEM((rows, inner), F32),
            pltpu.VMEM((chunks, height, 128), F32),
            pltpu.VMEM((chunks, height, 128), F32),
            pltpu.VMEM((groups - 1, 8, 128), jnp.int32),
            pltpu.SemaphoreType.DMA((chunks,)),
            pltpu.SemaphoreType.DMA((2, chunks)),
            pltpu.SemaphoreType.DMA((2, chunks)),
            pltpu.SemaphoreType.DMA((2, chunks * (team - 1))),
            pltpu.SemaphoreType.DMA((2, chunks)),
            pltpu.SemaphoreType.DMA((2, chunks * (2 * team - 1))),
            pltpu.SemaphoreType.DMA((2, chunks * 2 * team)),
            pltpu.SemaphoreType.DMA((2, groups - 1)),
        ],
        compiler_params=pltpu.CompilerParams(
            collective_id=0, has_side_effects=True, vmem_limit_bytes=32 * 1024 * 1024
        ),
    )(
        kept_scale,
        skip_gain,
        inner_proj,
        input_map,
        output_map,
        mix,
        keep,
        after,
        valid,
        cache_rows,
        value_kernel,
        value_offset.reshape(1, -1),
        out_gain.reshape(1, -1),
        own_total,
        out_weight,
        pinned(scan_state.reshape(requests, inner, state_size)),
    )
    group_rows = jnp.transpose(group_cache, (1, 0, 2))
    out_rows, kept_state, value_kept, group_kept = pl.pallas_call(
        finish_kernel,
        out_shape=[
            pltpu.HBM((rows, model_width), BF16),
            pltpu.HBM((requests, inner, state_size), BF16),
            pltpu.HBM((depth, requests, inner), BF16),
            pltpu.HBM((depth, requests, map_width), BF16),
        ],
        in_specs=[vmem] * 8,
        out_specs=[hbm] * 4,
        scratch_shapes=[
            pltpu.VMEM((depth, requests, inner), BF16),
            pltpu.VMEM((depth, requests, map_width), BF16),
            pltpu.SemaphoreType.DMA((10,)),
        ],
        compiler_params=pltpu.CompilerParams(vmem_limit_bytes=16 * 1024 * 1024),
    )(
        out_rows,
        kept_state,
        inner_proj,
        cache_rows,
        group_proj,
        group_rows,
        fresh_pick,
        cache_pick,
    )
    return (
        out_rows.reshape(requests, positions, model_width),
        kept_state.reshape(scan_state.shape),
        jnp.transpose(value_kept, (1, 0, 2)),
        jnp.transpose(group_kept, (1, 0, 2)),
        totals,
    )


def solution(mesh):
    placed = (
        P("dp", None, None),
        P(),
        P(None, None, "tensor"),
        P(None, "tensor"),
        P(None, "tensor"),
        P(None, "tensor"),
        P("tensor"),
        P(None, "tensor"),
        P("tensor"),
        P("tensor"),
        P("tensor"),
        P("tensor"),
        P("tensor"),
        P("tensor", None),
        P("dp", "tensor", None, None),
        P("dp", None, "tensor"),
        P("dp", None, "tensor"),
        P("dp"),
        P("dp"),
        P("dp"),
    )
    return jax.shard_map(
        local,
        mesh=mesh,
        in_specs=placed,
        out_specs=(
            P("dp", None, None),
            P("dp", "tensor", None, None),
            P("dp", None, "tensor"),
            P("dp", None, "tensor"),
            P(),
        ),
        check_vma=False,
    )
```
